256 devices in a mesh: segment: 16 (over z, x_lo), dp: 16 (over y, x_hi, core).
Axes of the slice: x: 4 (x_hi: 2, x_lo: 2; x = x_hi * 2 + x_lo), y: 4, z: 8, core: 2. Of those that a mesh axis runs over, the one named last changes fastest.
Arguments:
- src_embed: bfloat16 [64, 128, 2048], P('dp', None, 'segment'), parts along dimension 0, may hold values from -6 to 6
- tgt_embed: bfloat16 [64, 128, 2048], P('dp', None, 'segment'), parts along dimension 0, may hold values from -6 to 6
- src_lengths: int32 [64], P('dp'), parts along dimension 0, may hold values from 32 to 128
- tgt_lengths: int32 [64], P('dp'), parts along dimension 0, may hold values from 32 to 128
- attn_in: bfloat16 [16, 2048, 1536], P('segment'), may hold values from -0.125 to 0.125
- attn_out: bfloat16 [16, 512, 2048], P('segment'), may hold values from -0.375 to 0.375
- norm_gain: float32 [4, 2048], replicated, may hold values from 0.25 to 1.75
- final_gain: float32 [2048], replicated, may hold values from 0.25 to 1.75
Outputs:
- decoded: bfloat16 [64, 128, 2048], P('dp', None, 'segment'), parts along dimension 0
The draws below stay inside these ranges and needn't reach their ends.
There are 16 independent parts, one for each index of `dp`. The reference program is written for one: setup_inputs(seed, part) draws one part's arguments, and reference() takes and returns one part's arrays. A program takes and returns all parts, laid end to end along the dimension named above; an argument that names none is the same for every part. Nothing has to cross between parts.
Inputs may be any that keep to these rules, and one draw needn't show every extreme that they name: `src_lengths`: keys at positions below a sequence's length are its real tokens. `tgt_lengths`: keys at positions below a sequence's length are its real tokens.
All inputs are finite; a program needn't handle non-finite values.
Results may differ from the reference program's by a relative error of at most 0.015.
Values may be sent and summed in bfloat16 or wider, within the bound.
A program may use at most 64 MiB of HBM per device.

```python
import jax
import jax.numpy as jnp
from jax import lax

D = 2048
HEAD = 64
MB = 4
S = 128
GROUP = 4
INNER = 2048
N_SEGMENT = 16


def place_ends(drawn, key, smallest, top_value):
    shape = drawn.shape
    index_at = [jax.random.randint(jax.random.fold_in(key, axis), (), 0, shape[axis]) for axis in range(len(shape))]
    drawn = drawn.at[tuple(index_at)].set(smallest)
    longest = shape.index(max(shape))
    index_at[longest] = (index_at[longest] + 1) % shape[longest]
    return drawn.at[tuple(index_at)].set(top_value)


def block_levels(stream_key, extent, cuts, low, top_value):
    def one(axis_at, blocks):
        steps = jax.random.uniform(jax.random.fold_in(jax.random.fold_in(stream_key, 6), axis_at), (blocks,), jnp.float32, low / len(cuts), top_value / len(cuts))
        return jnp.repeat(jnp.exp(steps), extent[axis_at] // blocks).reshape((-1,) + (1,) * (len(extent) - axis_at - 1))

    gain = one(*cuts[0])
    for cut in cuts[1:]:
        gain = gain * one(*cut)
    return gain


def centred(own_key, shape, deviation, most, cuts=(), kind=jnp.bfloat16):
    array = jax.random.normal(own_key, shape, jnp.float32) * deviation
    if len(cuts) > 0:
        array = block_levels(own_key, shape, cuts, -0.22, 0.18) * array
    return jnp.clip(array, min=-most, max=most).astype(kind)


def setup_inputs(seed: int = 0, part: int = 0) -> dict:
    key_list = jax.random.split(jax.random.key(seed), 9)
    part_keys = jax.random.split(jax.random.fold_in(key_list[8], part), 9)
    return {
        "src_embed": centred(part_keys[0], (MB, S, D), 1.0, 6.0, ((2, 16),)),
        "tgt_embed": centred(part_keys[1], (MB, S, D), 1.0, 6.0, ((2, 16),)),
        "src_lengths": place_ends(jax.random.randint(part_keys[2], (MB,), S // 4, S + 1), jax.random.fold_in(part_keys[2], 1), S // 4, S).astype(jnp.int32),
        "tgt_lengths": place_ends(jax.random.randint(part_keys[3], (MB,), S // 4, S + 1), jax.random.fold_in(part_keys[3], 1), S // 4, S).astype(jnp.int32),
        "attn_in": centred(key_list[4], (N_SEGMENT, D, 3 * INNER // GROUP), D ** -0.5, 0.125, ((0, 16),)),
        "attn_out": centred(key_list[5], (N_SEGMENT, INNER // GROUP, D), (INNER // 8) ** -0.5, 0.375, ((0, 16),)),
        "norm_gain": jnp.clip(1.0 + 0.15 * jax.random.normal(key_list[6], (4, D), jnp.float32), 0.25, 1.75),
        "final_gain": jnp.clip(1.0 + 0.15 * jax.random.normal(key_list[7], (D,), jnp.float32), 0.25, 1.75),
    }


epsilon = 1e-06
score_scale = 0.125

def rms_scale(values, gain_vector):
    return values * lax.rsqrt(lax.optimization_barrier(jnp.mean(values * values, axis=-1, keepdims=True)) + epsilon) * gain_vector

def attention(queries, key_rows, values, allowed):
    head_count = queries.shape[1] // HEAD
    shaped_q = queries.reshape(queries.shape[0], head_count, HEAD).astype(jnp.float32)
    shaped_k = key_rows.reshape(key_rows.shape[0], head_count, HEAD).astype(jnp.float32)
    shaped_v = values.reshape(values.shape[0], head_count, HEAD).astype(jnp.float32)
    scores = jnp.einsum('qhd,khd->hqk', shaped_q, shaped_k) * score_scale
    scores = jnp.where(allowed[None], scores, -1000000000.0)
    weights = jax.nn.softmax(scores, axis=-1).astype(jnp.bfloat16)
    mixture = jnp.einsum('hqk,khd->qhd', weights.astype(jnp.float32), shaped_v)
    return mixture.reshape(queries.shape[0], -1).astype(jnp.bfloat16)

def sublayer(inputs, memory, attn_in, attn_out, norm_gain, layer_slot, group_size, allowed):
    normed = rms_scale(inputs.astype(jnp.float32), norm_gain[layer_slot]).astype(jnp.bfloat16)
    source = normed if memory is None else memory
    summed = jnp.zeros(inputs.shape, jnp.float32)
    for member in range(group_size):
        weight_slot = layer_slot * group_size + member
        in_weight = attn_in[weight_slot]
        out_weight = attn_out[weight_slot]
        head_cols = out_weight.shape[0]
        queries = jnp.dot(normed, in_weight[:, :head_cols], preferred_element_type=jnp.float32).astype(jnp.bfloat16)
        key_value = jnp.dot(source, in_weight[:, head_cols:], preferred_element_type=jnp.float32).astype(jnp.bfloat16)
        mixture = attention(queries, key_value[:, :head_cols], key_value[:, head_cols:], allowed)
        summed = summed + jnp.dot(mixture, out_weight, preferred_element_type=jnp.float32)
    return (inputs.astype(jnp.float32) + summed).astype(jnp.bfloat16)

def reference(src_embed, tgt_embed, src_lengths, tgt_lengths, attn_in, attn_out, norm_gain, final_gain):
    group_size = N_SEGMENT // 4
    positions = jnp.arange(S, dtype=jnp.int32)
    causal = positions[None, :] <= positions[:, None]
    results = []
    for batch_slot in range(MB):
        source_ok = jnp.broadcast_to(positions[None, :] < src_lengths[batch_slot], (S, S))
        target_ok = (positions[None, :] < tgt_lengths[batch_slot]) & causal
        encoded = src_embed[batch_slot]
        for layer_slot in range(2):
            encoded = sublayer(encoded, None, attn_in, attn_out, norm_gain, layer_slot, group_size, source_ok)
        memory = rms_scale(encoded.astype(jnp.float32), final_gain).astype(jnp.bfloat16)
        decoded = sublayer(tgt_embed[batch_slot], memory, attn_in, attn_out, norm_gain, 2, group_size, source_ok)
        decoded = sublayer(decoded, None, attn_in, attn_out, norm_gain, 3, group_size, target_ok)
        results.append(decoded)
    return jnp.stack(results)
```

```python
import functools

import jax
import jax.numpy as jnp
from jax import lax
from jax.experimental import pallas as pl
from jax.experimental.pallas import tpu as pltpu
from jax.sharding import PartitionSpec as P

HEAD = 64
GROUP = 4
EPS = 1e-06
SCALE = 0.125
MASKED = -1000000000.0
MESH = pl.DeviceIdType.MESH
F32 = jnp.float32
BF16 = jnp.bfloat16


def rms(values, gain):
    return values * lax.rsqrt(jnp.mean(values * values, axis=-1, keepdims=True) + EPS) * gain


def kernel(
    n_seg, src, tgt, slen, tlen, win, wout, gain, fgain, out,
    w_in, w_out, arr, tg, nb, sb, qkv, mix, pf, part, rx, rz, zs, yb,
    wsem, src_send, tgt_send, arr_recv, tgt_recv,
    relay_s, relay_r, agz_s, agz_r, agx_s, agx_r, rsx_s, rsx_r, rsz_s, rsz_r, out_s, out_r,
):
    batches, seq, cols = src.shape
    rows = seq // GROUP
    heads = w_out.shape[0]
    s = lax.axis_index("segment")
    sect = s // GROUP
    m = s % GROUP
    zl = m // 2
    xl = m % 2
    x_near = s + 1 - 2 * xl
    z_near = s + 2 - 4 * zl
    last = n_seg // GROUP - 1

    load_in = pltpu.make_async_copy(win.at[0], w_in, wsem.at[0])
    load_out = pltpu.make_async_copy(wout.at[0], w_out, wsem.at[1])
    load_in.start()
    load_out.start()

    barrier = pltpu.get_barrier_semaphore()
    for k in range(1, n_seg):
        pl.semaphore_signal(
            barrier, inc=1, device_id={"segment": (s + k) % n_seg}, device_id_type=MESH
        )
    pl.semaphore_wait(barrier, n_seg - 1)

    def remote(src_ref, dst_ref, send, recv, target):
        return pltpu.make_async_remote_copy(
            src_ref=src_ref, dst_ref=dst_ref, send_sem=send, recv_sem=recv,
            device_id={"segment": target}, device_id_type=MESH,
        )

    def wait_for(ref, sem):
        pltpu.make_async_copy(ref, ref, sem).wait()

    def quarter(q):
        return pl.ds(pl.multiple_of(q * rows, rows), rows)

    own_cols = pl.ds(pl.multiple_of(s * cols, cols), cols)

    def scatter(given, held, send, recv, first):
        def one(b, carry):
            for t in range(GROUP):
                @pl.when(s != first + t)
                def _():
                    remote(
                        given.at[b], held.at[b, :, own_cols], send.at[b, t], recv.at[b], first + t
                    ).start()

                @pl.when(s == first + t)
                def _():
                    pltpu.make_async_copy(given.at[b], held.at[b, :, own_cols], recv.at[b]).start()
            return carry

        lax.fori_loop(0, batches, one, 0)

    scatter(src, arr, src_send, arr_recv, 0)
    scatter(tgt, tg, tgt_send, tgt_recv, 2 * GROUP)

    def relay(b):
        return remote(
            yb.at[b], arr.at[b, quarter(m)], relay_s.at[b], relay_r.at[b], (s + GROUP) % n_seg
        )

    def gather_z(b):
        part_ref = arr.at[b, quarter(m)]
        return remote(part_ref, part_ref, agz_s.at[b], agz_r.at[b], z_near)

    def gather_x(b, which):
        part_ref = arr.at[b, quarter(m if which == 0 else z_near % GROUP)]
        return remote(part_ref, part_ref, agx_s.at[b, which], agx_r.at[b, which], x_near)

    def sum_x(b, which):
        wanted = x_near % GROUP
        if which == 0:
            wanted = (wanted + 2) % GROUP
        return remote(
            part.at[b, quarter(wanted)], rx.at[b, which], rsx_s.at[b, which], rsx_r.at[b, which], x_near
        )

    def sum_z(b):
        return remote(zs.at[b], rz.at[b], rsz_s.at[b], rsz_r.at[b], z_near)

    def out_copy(b, t):
        return remote(
            yb.at[b, :, pl.ds(pl.multiple_of(t * cols, cols), cols)],
            out.at[b, quarter(m)], out_s.at[b, t], out_r.at[b], t,
        )

    def step_r(b):
        wait_for(arr.at[b, quarter(m)], relay_r.at[b])
        gather_z(b).start()
        gather_x(b, 0).start()

    def step_f(b):
        gather_z(b).wait_recv()
        gather_x(b, 1).start()

    def step_c(b):
        @pl.when(sect == 0)
        def _():
            wait_for(arr.at[b], arr_recv.at[b])

        @pl.when(sect > 0)
        def _():
            gather_x(b, 0).wait_recv()
            gather_x(b, 1).wait_recv()

        own_gain = gain[pl.ds(sect, 1), :]

        @pl.when(sect == 2)
        def _():
            wait_for(tg.at[b], tgt_recv.at[b])
            nb[...] = rms(tg[b].astype(F32), own_gain).astype(BF16)
            sb[...] = arr[b]

        @pl.when(sect != 2)
        def _():
            normed = rms(arr[b].astype(F32), own_gain).astype(BF16)
            nb[...] = normed
            sb[...] = normed

        qkv[:, :heads] = jnp.dot(
            nb[...], w_in[:, :heads], preferred_element_type=F32
        ).astype(BF16)
        qkv[:, heads:] = jnp.dot(
            sb[...], w_in[:, heads:], preferred_element_type=F32
        ).astype(BF16)

        length = jnp.where(sect == last, tlen[b], slen[b])
        query_pos = lax.broadcasted_iota(jnp.int32, (seq, seq), 0)
        key_pos = lax.broadcasted_iota(jnp.int32, (seq, seq), 1)
        limit = jnp.where(sect == last, query_pos, seq)
        allowed = (key_pos < length) & (key_pos <= limit)
        allowed = jnp.concatenate([allowed, allowed], axis=0)
        pair = 2 * HEAD
        low = lax.broadcasted_iota(jnp.int32, (seq, pair), 1) < HEAD
        for j in range(heads // pair):
            q2 = qkv[:, j * pair:(j + 1) * pair]
            k2 = qkv[:, heads + j * pair:heads + (j + 1) * pair]
            v2 = qkv[:, 2 * heads + j * pair:2 * heads + (j + 1) * pair]
            zero = jnp.zeros_like(q2)
            stacked = jnp.concatenate([jnp.where(low, q2, zero), jnp.where(low, zero, q2)], axis=0)
            scores = lax.dot_general(
                stacked, k2, (((1,), (1,)), ((), ())), preferred_element_type=F32
            ) * SCALE
            scores = jnp.where(allowed, scores, MASKED)
            grown = jnp.exp(scores - jnp.max(scores, axis=-1, keepdims=True))
            weights = (grown / jnp.sum(grown, axis=-1, keepdims=True)).astype(BF16)
            both = jnp.dot(weights, v2, preferred_element_type=F32)
            mix[:, j * pair:(j + 1) * pair] = jnp.where(low, both[:seq], both[seq:]).astype(BF16)

        total = jnp.dot(mix[...], w_out[...], preferred_element_type=F32)
        pf[...] = total
        part[b] = total.astype(BF16)
        sum_x(b, 0).start()
        sum_x(b, 1).start()

    def step_z(b):
        sum_x(b, 0).wait_recv()
        zs[b] = (pf[quarter(z_near % GROUP), :] + rx[b, 0].astype(F32)).astype(BF16)
        sum_z(b).start()

    def step_y(b):
        sum_x(b, 1).wait_recv()
        sum_z(b).wait_recv()
        total = pf[quarter(m), :] + rx[b, 1].astype(F32) + rz[b].astype(F32)

        @pl.when(sect == 2)
        def _():
            yb[b] = (tg[b, quarter(m), :].astype(F32) + total).astype(BF16)

        @pl.when(sect == 1)
        def _():
            encoded = (arr[b, quarter(m), :].astype(F32) + total).astype(BF16)
            yb[b] = rms(encoded.astype(F32), fgain[...]).astype(BF16)

        @pl.when((sect != 1) & (sect != 2))
        def _():
            yb[b] = (arr[b, quarter(m), :].astype(F32) + total).astype(BF16)

        @pl.when(sect < last)
        def _():
            relay(b).start()

        @pl.when(sect == last)
        def _():
            def one(t, carry):
                @pl.when(t != s)
                def _():
                    out_copy(b, t).start()

                @pl.when(t == s)
                def _():
                    pltpu.make_async_copy(yb.at[b, :, own_cols], out.at[b, quarter(m)], out_r.at[b]).start()
                return carry

            lax.fori_loop(0, n_seg, one, 0)

    load_in.wait()
    load_out.wait()

    @pl.when(sect > 0)
    def _():
        step_r(0)
        step_f(0)

    def main(b, carry):
        step_c(b)

        @pl.when((sect > 0) & (b < batches - 1))
        def _():
            step_r(b + 1)

        step_z(b)

        @pl.when((sect > 0) & (b < batches - 1))
        def _():
            step_f(b + 1)

        step_y(b)
        return carry

    lax.fori_loop(0, batches, main, 0)

    def finish(b, carry):
        for t in range(GROUP):
            @pl.when(s != t)
            def _():
                remote(src.at[b], arr.at[b, :, own_cols], src_send.at[b, t], arr_recv.at[b], t).wait_send()

            @pl.when(s != 2 * GROUP + t)
            def _():
                remote(
                    tgt.at[b], tg.at[b, :, own_cols], tgt_send.at[b, t], tgt_recv.at[b], 2 * GROUP + t
                ).wait_send()

        sum_x(b, 0).wait_send()
        sum_x(b, 1).wait_send()
        sum_z(b).wait_send()

        @pl.when(sect > 0)
        def _():
            gather_z(b).wait_send()
            gather_x(b, 0).wait_send()
            gather_x(b, 1).wait_send()

        @pl.when(sect < last)
        def _():
            relay(b).wait_send()

        @pl.when(sect == last)
        def _():
            def one(t, inner):
                @pl.when(t != s)
                def _():
                    out_copy(b, t).wait_send()
                return inner

            lax.fori_loop(0, n_seg, one, 0)

        wait_for(out.at[b], out_r.at[b])
        return carry

    lax.fori_loop(0, batches, finish, 0)


def on_device(n_seg, src, tgt, slen, tlen, win, wout, gain, fgain):
    batches, seq, cols = src.shape
    width = cols * n_seg
    depth, fan = win.shape[1:]
    heads = wout.shape[1]
    rows = seq // GROUP
    any_space = pl.BlockSpec(memory_space=pl.ANY)
    vmem = pl.BlockSpec(memory_space=pltpu.VMEM)
    smem = pl.BlockSpec(memory_space=pltpu.SMEM)
    dma = pltpu.SemaphoreType.DMA
    return pl.pallas_call(
        functools.partial(kernel, n_seg),
        out_shape=jax.ShapeDtypeStruct((batches, seq, cols), BF16),
        in_specs=[any_space, any_space, smem, smem, any_space, any_space, vmem, vmem],
        out_specs=any_space,
        scratch_shapes=[
            pltpu.VMEM((depth, fan), BF16),
            pltpu.VMEM((heads, width), BF16),
            pltpu.VMEM((batches, seq, width), BF16),
            pltpu.VMEM((batches, seq, width), BF16),
            pltpu.VMEM((seq, width), BF16),
            pltpu.VMEM((seq, width), BF16),
            pltpu.VMEM((seq, fan), BF16),
            pltpu.VMEM((seq, heads), BF16),
            pltpu.VMEM((seq, width), F32),
            pltpu.VMEM((batches, seq, width), BF16),
            pltpu.VMEM((batches, 2, rows, width), BF16),
            pltpu.VMEM((batches, rows, width), BF16),
            pltpu.VMEM((batches, rows, width), BF16),
            pltpu.VMEM((batches, rows, width), BF16),
            dma((2,)),
            dma((batches, GROUP)), dma((batches, GROUP)), dma((batches,)), dma((batches,)),
            dma((batches,)), dma((batches,)), dma((batches,)), dma((batches,)),
            dma((batches, 2)), dma((batches, 2)), dma((batches, 2)), dma((batches, 2)),
            dma((batches,)), dma((batches,)), dma((batches, n_seg)), dma((batches,)),
        ],
        compiler_params=pltpu.CompilerParams(
            collective_id=0, has_side_effects=True, vmem_limit_bytes=56 * 1024 * 1024
        ),
    )(src, tgt, slen, tlen, win, wout, gain, fgain.reshape(1, -1))


def solution(mesh):
    spec = P("dp", None, "segment")
    return jax.shard_map(
        functools.partial(on_device, mesh.shape["segment"]),
        mesh=mesh,
        in_specs=(spec, spec, P("dp"), P("dp"), P("segment", None, None), P("segment", None, None), P(), P()),
        out_specs=spec,
        check_vma=False,
    )
```

```python
import functools

import jax
import jax.numpy as jnp
from jax import lax
from jax.experimental import pallas as pl
from jax.experimental.pallas import tpu as pltpu
from jax.sharding import PartitionSpec as P

HEAD = 64
GROUP = 4
CHUNKS = 4
AHEAD = 1
EARLY = 0
EPS = 1e-06
SCALE = 0.125
MASKED = -1000000000.0
MESH = pl.DeviceIdType.MESH
F32 = jnp.float32
BF16 = jnp.bfloat16


def rms(values, gain):
    return values * lax.rsqrt(jnp.mean(values * values, axis=-1, keepdims=True) + EPS) * gain


def kernel(
    n_seg, n_dp, src, tgt, slen, tlen, win, wout, gain, fgain, out,
    w_in, w_out, w_far, lens_own, lens_far, lens, arr, tg, nb, qs, qkv, mix, mix_far, pf, part, rx, rz, zs, yb,
    wsem, lens_s, lens_r, far_s, far_r, mix_s, mix_r, src_s, tgt_s, src_r, tgt_r, tz_s, tz_r, tx_s, tx_r,
    relay_s, relay_r, agz_s, agz_r, agx_s, agx_r, rsx_s, rsx_r, rsz_s, rsz_r, out_s, out_r,
):
    batches, seq, cols = src.shape
    rows = seq // GROUP
    half = seq // 2
    block = cols * n_seg // CHUNKS
    heads = w_out.shape[0]
    s = lax.axis_index("segment")
    sect = s // GROUP
    m = s % GROUP
    zl = m // 2
    xl = m % 2
    x_near = s + 1 - 2 * xl
    d = lax.axis_index("dp")
    flipped = d + 2 - 4 * ((d // 2) % 2)
    alt = d % 2 == 1
    swap = alt & (xl == 0)
    x_dp = jnp.where(alt, flipped, d)
    work_dp = jnp.where(swap, flipped, d)
    core = d % 2
    twin = d + 1 - 2 * core
    own_q = xl * 2 + zl
    z_q = xl * 2 + 1 - zl
    lower = (sect > 0) & (zl == 0)
    upper = (sect > 0) & (zl == 1)
    z_near = s + 2 - 4 * zl
    last = n_seg // GROUP - 1

    load_in = pltpu.make_async_copy(win.at[0], w_in, wsem.at[0])
    load_out = pltpu.make_async_copy(wout.at[0], w_out, wsem.at[1])
    load_in.start()
    load_out.start()

    barrier = pltpu.get_barrier_semaphore()
    for k in range(1, n_seg):
        pl.semaphore_signal(
            barrier, inc=1, device_id={"segment": (s + k) % n_seg}, device_id_type=MESH
        )

    pl.semaphore_signal(
        barrier, inc=1, device_id={"segment": s, "dp": twin}, device_id_type=MESH
    )

    for k in range(1, n_dp // 4):
        pl.semaphore_signal(
            barrier, inc=1, device_id={"segment": s, "dp": (d + 4 * k) % n_dp}, device_id_type=MESH
        )

    @pl.when(alt)
    def _():
        for k in range(n_seg):
            pl.semaphore_signal(
                barrier, inc=1, device_id={"segment": k, "dp": flipped}, device_id_type=MESH
            )

    row = lax.broadcasted_iota(jnp.int32, lens_own.shape, 0)
    table = jnp.zeros(lens_own.shape, F32)
    for k in range(batches):
        table = jnp.where(row == k, slen[k].astype(F32), table)
        table = jnp.where(row == batches + k, tlen[k].astype(F32), table)
    lens_own[...] = table
    with jax.named_scope("barrier"):
        pl.semaphore_wait(barrier, n_seg + n_dp // 4 - 1 + jnp.where(alt, n_seg, 0))

    def remote(src_ref, dst_ref, send, recv, target, target_dp=None):
        return pltpu.make_async_remote_copy(
            src_ref=src_ref, dst_ref=dst_ref, send_sem=send, recv_sem=recv,
            device_id={"segment": target, "dp": d if target_dp is None else target_dp},
            device_id_type=MESH,
        )

    def lens_copy():
        return remote(lens_own, lens_far, lens_s, lens_r, s, flipped)

    @pl.when(swap)
    def _():
        lens_copy().start()

    def wait_for(ref, sem):
        pltpu.make_async_copy(ref, ref, sem).wait()

    def quarter(q):
        return pl.ds(pl.multiple_of(q * rows, rows), rows)

    def strip(c):
        return slice(c * block, (c + 1) * block)

    tall = n_dp // 4
    share = heads // (2 * tall)
    y = d // 4

    def far_rows(level):
        return pl.ds(pl.multiple_of((core * tall + level) * share, share), share)

    def far_copy():
        return remote(wout.at[0, far_rows(y)], w_far.at[far_rows(y)], far_s.at[0], far_r.at[0], z_near)

    def far_side(k):
        ref = w_far.at[far_rows(y)]
        return remote(ref, ref, far_s.at[k], far_r.at[k], s, (d + 4 * k) % n_dp)

    def far_swap():
        ref = w_far.at[pl.ds(pl.multiple_of(core * (heads // 2), heads // 2), heads // 2)]
        return remote(ref, ref, far_s.at[tall], far_r.at[tall], s, twin)

    own_cols = pl.ds(pl.multiple_of(s * cols, cols), cols)

    def part_of(t):
        return slice((t % 2 * 2 + t // 2) * rows, (t % 2 * 2 + t // 2 + 1) * rows)

    def spread(given, held, send, recv, first, b, t):
        return remote(
            given.at[b, part_of(t)], held.at[b, part_of(t), own_cols],
            send.at[b, t], recv.at[b], first + t,
            jnp.where(alt, flipped, d) if t % 2 == 0 else d,
        )

    def stays(first, t):
        same = s == first + t
        return same & jnp.logical_not(alt) if t % 2 == 0 else same

    def scatter(given, held, send, recv, first, b):
        for t in range(GROUP):
            @pl.when(jnp.logical_not(stays(first, t)))
            def _():
                spread(given, held, send, recv, first, b, t).start()

            @pl.when(stays(first, t))
            def _():
                pltpu.make_async_copy(
                    given.at[b, part_of(t)], held.at[b, part_of(t), own_cols], recv.at[b]
                ).start()

    def scattered(given, held, send, recv, first, b):
        for t in range(GROUP):
            @pl.when(jnp.logical_not(stays(first, t)))
            def _():
                spread(given, held, send, recv, first, b, t).wait_send()

    def give_source(b, carry):
        scatter(src, arr, src_s, src_r, 0, b)
        return carry

    @pl.when(lower & (sect == 1))
    def _():
        far_copy().start()

    give_source(0, 0)

    @pl.when(sect > 0)
    def _():
        scattered(src, arr, src_s, src_r, 0, 0)

    lax.fori_loop(1, batches, give_source, 0)

    @pl.when(lower & (sect > 1))
    def _():
        far_copy().start()

    def give_target(b, carry):
        scatter(tgt, tg, tgt_s, tgt_r, 2 * GROUP, b)
        return carry

    lax.fori_loop(0, batches, give_target, 0)

    def side_rows(side):
        return pl.ds(pl.multiple_of(side * half, half), half)

    def relay_first(b, c):
        return remote(
            yb.at[b, :rows, strip(c)], arr.at[b, quarter(own_q), strip(c)], relay_s.at[b, c],
            relay_r.at[b, c], GROUP + xl,
        )

    def relay(b, c):
        return remote(
            yb.at[b, :, strip(c)], arr.at[b, side_rows(xl), strip(c)],
            relay_s.at[b, c], relay_r.at[b, c], (s + 2) % n_seg,
        )

    def gather_z(b, c):
        ref = arr.at[b, quarter(own_q), strip(c)]
        return remote(ref, ref, agz_s.at[b, c], agz_r.at[b, c], z_near)

    def gather_x(b, which, c):
        ref = arr.at[b, quarter(own_q if which == 0 else z_q), strip(c)]
        return remote(ref, ref, agx_s.at[b, which, c], agx_r.at[b, which, c], x_near, x_dp)

    def lift_z(b, c):
        ref = arr.at[b, side_rows(xl), strip(c)]
        return remote(ref, ref, agz_s.at[b, c], agz_r.at[b, c], z_near)

    def half_x(b, c):
        ref = arr.at[b, side_rows(xl), strip(c)]
        return remote(ref, ref, agx_s.at[b, 0, c], agx_r.at[b, 0, c], x_near, x_dp)

    def mix_z(b):
        return remote(mix.at[b], mix_far.at[b], mix_s.at[b], mix_r.at[b], z_near)

    def target_z(b):
        ref = tg.at[b, quarter(own_q)]
        return remote(ref, ref, tz_s.at[b], tz_r.at[b], z_near)

    def target_x(b, which):
        ref = tg.at[b, quarter(own_q if which == 0 else z_q)]
        return remote(ref, ref, tx_s.at[b, which], tx_r.at[b, which], x_near, x_dp)

    def sum_x(b, which, c):
        wanted = (1 - xl) * 2 + (1 - zl if which == 0 else zl)
        return remote(
            part.at[b, quarter(wanted), strip(c)], rx.at[b, which * rows:(which + 1) * rows, strip(c)],
            rsx_s.at[b, which, c], rsx_r.at[b, which, c], x_near, x_dp,
        )

    def sum_half(b, c):
        return remote(
            part.at[b, side_rows(1 - xl), strip(c)], rx.at[b, :, strip(c)],
            rsx_s.at[b, 0, c], rsx_r.at[b, 0, c], x_near, x_dp,
        )

    def sum_z(b, c):
        return remote(zs.at[b, :, strip(c)], rz.at[b, :, strip(c)], rsz_s.at[b, c], rsz_r.at[b, c], z_near)

    def out_copy(b, t):
        return remote(
            yb.at[b, :, pl.ds(pl.multiple_of(t * cols, cols), cols)],
            out.at[b, pl.ds(pl.multiple_of(xl * half, half), half)], out_s.at[b, t], out_r.at[b], t, work_dp,
        )

    def step_r(b):
        with jax.named_scope("r_wait"):
            wait_for(arr.at[b, quarter(own_q)], src_r.at[b])
        for c in range(CHUNKS):
            gather_z(b, c).start()
            gather_x(b, 0, c).start()

    def step_f(b, c):
        with jax.named_scope("f_wait"):
            gather_z(b, c).wait_recv()
        gather_x(b, 1, c).start()

    def step_r2(b, c):
        with jax.named_scope("r_wait"):
            wait_for(arr.at[b, side_rows(xl), strip(c)], relay_r.at[b, c])
        lift_z(b, c).start()
        half_x(b, c).start()

    def step_f2(b, c):
        with jax.named_scope("f_wait"):
            lift_z(b, c).wait_recv()
        half_x(b, c).start()

    own_gain = gain[pl.ds(sect, 1), :]

    def attend(b):
        @pl.when(sect == 2)
        def _():
            qkv[:, :heads] = qs[b]
            nb[...] = rms(arr[b].astype(F32), fgain[...]).astype(BF16)

        @pl.when(sect != 2)
        def _():
            nb[...] = rms(arr[b].astype(F32), own_gain).astype(BF16)
            qkv[:, :heads] = jnp.dot(
                nb[...], w_in[:, :heads], preferred_element_type=F32
            ).astype(BF16)

        with jax.named_scope("kv_dot"):
            qkv[:, heads:] = jnp.dot(
                nb[...], w_in[:, heads:], preferred_element_type=F32
            ).astype(BF16)

        length = lens[pl.ds(jnp.where(sect == last, batches, 0) + b, 1), :seq]
        query_pos = lax.broadcasted_iota(jnp.int32, (seq, seq), 0)
        key_pos = lax.broadcasted_iota(jnp.int32, (seq, seq), 1)
        limit = jnp.where(sect == last, query_pos, seq)
        allowed = (key_pos.astype(F32) < length) & (key_pos <= limit)
        allowed = jnp.concatenate([allowed, allowed], axis=0)
        pair = 2 * HEAD
        low = lax.broadcasted_iota(jnp.int32, (seq, pair), 1) < HEAD
        for j in range(heads // pair):
            q2 = qkv[:, j * pair:(j + 1) * pair]
            k2 = qkv[:, heads + j * pair:heads + (j + 1) * pair]
            v2 = qkv[:, 2 * heads + j * pair:2 * heads + (j + 1) * pair]
            zero = jnp.zeros_like(q2)
            stacked = jnp.concatenate([jnp.where(low, q2, zero), jnp.where(low, zero, q2)], axis=0)
            scores = lax.dot_general(
                stacked, k2, (((1,), (1,)), ((), ())), preferred_element_type=F32
            ) * SCALE
            scores = jnp.where(allowed, scores, MASKED)
            grown = jnp.exp(scores - jnp.max(scores, axis=-1, keepdims=True))
            weights = (grown / jnp.sum(grown, axis=-1, keepdims=True)).astype(BF16)
            both = jnp.dot(weights, v2, preferred_element_type=F32)
            mix[b, :, j * pair:(j + 1) * pair] = jnp.where(low, both[:seq], both[seq:]).astype(BF16)

    def step_z(b, c):
        with jax.named_scope("z_wait"):
            sum_x(b, 0, c).wait_recv()
        zs[b, :, strip(c)] = (pf[quarter(z_q), strip(c)] + rx[b, :rows, strip(c)].astype(F32)).astype(BF16)
        sum_z(b, c).start()

    def step_y(b, c):
        with jax.named_scope("y_wait"):
            sum_x(b, 1, c).wait_recv()
            sum_z(b, c).wait_recv()
        total = (
            pf[quarter(own_q), strip(c)] + rx[b, rows:, strip(c)].astype(F32)
            + rz[b, :, strip(c)].astype(F32)
        )
        yb[b, :rows, strip(c)] = (arr[b, quarter(own_q), strip(c)].astype(F32) + total).astype(BF16)
        relay_first(b, c).start()

    def step_y2(b, c):
        with jax.named_scope("y_wait"):
            sum_half(b, c).wait_recv()
        mine = side_rows(xl)
        total = pf[mine, strip(c)] + rx[b, :, strip(c)].astype(F32)

        @pl.when(sect == 2)
        def _():
            yb[b, :, strip(c)] = (tg[b, mine, strip(c)].astype(F32) + total).astype(BF16)

        @pl.when(sect != 2)
        def _():
            yb[b, :, strip(c)] = (arr[b, mine, strip(c)].astype(F32) + total).astype(BF16)

        @pl.when(sect < last)
        def _():
            relay(b, c).start()

        if c == CHUNKS - 1:
            @pl.when(sect == last)
            def _():
                def one(t, carry):
                    @pl.when((t != s) | swap)
                    def _():
                        out_copy(b, t).start()

                    @pl.when((t == s) & jnp.logical_not(swap))
                    def _():
                        pltpu.make_async_copy(
                            yb.at[b, :, own_cols],
                            out.at[b, pl.ds(pl.multiple_of(xl * half, half), half)], out_r.at[b],
                        ).start()
                    return carry

                lax.fori_loop(0, n_seg, one, 0)

    @pl.when(swap)
    def _():
        lens_copy().wait()
        lens[...] = lens_far[...]

    @pl.when(jnp.logical_not(swap))
    def _():
        lens[...] = lens_own[...]

    with jax.named_scope("load"):
        load_in.wait()
        load_out.wait()

    @pl.when(sect == 2)
    def _():
        def first(b, carry):
            wait_for(tg.at[b, quarter(own_q)], tgt_r.at[b])
            target_z(b).start()
            target_x(b, 0).start()
            return carry

        lax.fori_loop(0, batches, first, 0)

        def second(b, carry):
            target_z(b).wait_recv()
            target_x(b, 1).start()
            return carry

        lax.fori_loop(0, batches, second, 0)

        def third(b, carry):
            target_x(b, 0).wait_recv()
            target_x(b, 1).wait_recv()
            nb[...] = rms(tg[b].astype(F32), own_gain).astype(BF16)
            qs[b] = jnp.dot(nb[...], w_in[:, :heads], preferred_element_type=F32).astype(BF16)
            return carry

        with jax.named_scope("target_q"):
            lax.fori_loop(0, batches, third, 0)

    @pl.when(upper)
    def _():
        with jax.named_scope("far"):
            far_copy().wait_recv()
            for k in range(1, tall):
                far_side(k).start()
            for k in range(1, tall):
                wait_for(w_far.at[far_rows((y + tall - k) % tall)], far_r.at[k])
            far_swap().start()

    @pl.when(sect == 0)
    def _():
        step_r(0)
        for c in range(CHUNKS):
            step_f(0, c)

    @pl.when(upper)
    def _():
        for c in range(CHUNKS):
            step_f2(0, c)
        far_swap().wait_recv()

    def main(b, carry):
        more = b < batches - 1

        @pl.when(lower)
        def _():
            for c in range(CHUNKS):
                step_r2(b, c)

        with jax.named_scope("c_wait"):
            @pl.when(sect == 0)
            def _():
                for c in range(CHUNKS):
                    gather_x(b, 0, c).wait_recv()
                    gather_x(b, 1, c).wait_recv()

            @pl.when(sect > 0)
            def _():
                for c in range(CHUNKS):
                    half_x(b, c).wait_recv()

        @pl.when(more & (sect == 0))
        def _():
            step_r(b + 1)

        attend(b)

        @pl.when(lower)
        def _():
            mix_z(b).start()

        @pl.when(sect == 0)
        def _():
            for c in range(CHUNKS):
                with jax.named_scope("out_dot"):
                    total = jnp.dot(mix[b], w_out[:, strip(c)], preferred_element_type=F32)
                    pf[:, strip(c)] = total
                    part[b, :, strip(c)] = total.astype(BF16)
                sum_x(b, 0, c).start()
                sum_x(b, 1, c).start()

            @pl.when(more)
            def _():
                for c in range(CHUNKS):
                    step_f(b + 1, c)

            for c in range(CHUNKS):
                step_z(b, c)
            for c in range(CHUNKS):
                step_y(b, c)

        @pl.when(upper)
        def _():
            @pl.when(more)
            def _():
                for c in range(EARLY):
                    step_f2(b + 1, c)

            with jax.named_scope("mix_wait"):
                mix_z(b).wait_recv()
            for c in range(CHUNKS):
                with jax.named_scope("out_dot2"):
                    total = jnp.dot(mix[b], w_out[:, strip(c)], preferred_element_type=F32)
                    total = total + jnp.dot(mix_far[b], w_far[:, strip(c)], preferred_element_type=F32)
                    pf[:, strip(c)] = total
                    part[b, :, strip(c)] = total.astype(BF16)
                sum_half(b, c).start()

            @pl.when(more)
            def _():
                for c in range(EARLY, AHEAD):
                    step_f2(b + 1, c)

            for c in range(CHUNKS):
                if c + AHEAD < CHUNKS:
                    @pl.when(more)
                    def _():
                        step_f2(b + 1, c + AHEAD)

                step_y2(b, c)
        return carry

    lax.fori_loop(0, batches, main, 0)

    def finish(b, carry):
        @pl.when((sect == 0) | (b > 0))
        def _():
            scattered(src, arr, src_s, src_r, 0, b)

        scattered(tgt, tg, tgt_s, tgt_r, 2 * GROUP, b)
        for c in range(CHUNKS):
            @pl.when(sect == 0)
            def _():
                sum_x(b, 0, c).wait_send()
                sum_x(b, 1, c).wait_send()
                sum_z(b, c).wait_send()
                gather_z(b, c).wait_send()
                gather_x(b, 0, c).wait_send()
                gather_x(b, 1, c).wait_send()
                relay_first(b, c).wait_send()

            @pl.when(lower)
            def _():
                lift_z(b, c).wait_send()
                half_x(b, c).wait_send()

            @pl.when(upper)
            def _():
                half_x(b, c).wait_send()
                sum_half(b, c).wait_send()

            @pl.when(upper & (sect < last))
            def _():
                relay(b, c).wait_send()

        @pl.when(lower)
        def _():
            mix_z(b).wait_send()

        @pl.when(sect == 2)
        def _():
            target_z(b).wait_send()
            target_x(b, 0).wait_send()
            target_x(b, 1).wait_send()

        @pl.when(upper & (sect == last))
        def _():
            def one(t, inner):
                @pl.when((t != s) | swap)
                def _():
                    out_copy(b, t).wait_send()
                return inner

            lax.fori_loop(0, n_seg, one, 0)

        with jax.named_scope("o_wait"):
            wait_for(out.at[b], out_r.at[b])
        return carry

    lax.fori_loop(0, batches, finish, 0)

    @pl.when(lower)
    def _():
        far_copy().wait_send()

    @pl.when(upper)
    def _():
        far_swap().wait_send()
        for k in range(1, tall):
            far_side(k).wait_send()


def on_device(n_seg, n_dp, src, tgt, slen, tlen, win, wout, gain, fgain):
    batches, seq, cols = src.shape
    width = cols * n_seg
    depth, fan = win.shape[1:]
    heads = wout.shape[1]
    rows = seq // GROUP
    any_space = pl.BlockSpec(memory_space=pl.ANY)
    vmem = pl.BlockSpec(memory_space=pltpu.VMEM)
    smem = pl.BlockSpec(memory_space=pltpu.SMEM)
    dma = pltpu.SemaphoreType.DMA
    return pl.pallas_call(
        functools.partial(kernel, n_seg, n_dp),
        out_shape=jax.ShapeDtypeStruct((batches, seq, cols), BF16),
        in_specs=[any_space, any_space, smem, smem, any_space, any_space, vmem, vmem],
        out_specs=any_space,
        scratch_shapes=[
            pltpu.VMEM((depth, fan), BF16),
            pltpu.VMEM((heads, width), BF16),
            pltpu.VMEM((heads, width), BF16),
            pltpu.VMEM((2 * batches, 128), F32),
            pltpu.VMEM((2 * batches, 128), F32),
            pltpu.VMEM((2 * batches, 128), F32),
            pltpu.VMEM((batches, seq, width), BF16),
            pltpu.VMEM((batches, seq, width), BF16),
            pltpu.VMEM((seq, width), BF16),
            pltpu.VMEM((batches, seq, heads), BF16),
            pltpu.VMEM((seq, fan), BF16),
            pltpu.VMEM((batches, seq, heads), BF16),
            pltpu.VMEM((batches, seq, heads), BF16),
            pltpu.VMEM((seq, width), F32),
            pltpu.VMEM((batches, seq, width), BF16),
            pltpu.VMEM((batches, 2 * rows, width), BF16),
            pltpu.VMEM((batches, rows, width), BF16),
            pltpu.VMEM((batches, rows, width), BF16),
            pltpu.VMEM((batches, 2 * rows, width), BF16),
            dma((2,)), dma, dma, dma((n_dp // 4 + 1,)), dma((n_dp // 4 + 1,)), dma((batches,)), dma((batches,)),
            dma((batches, GROUP)), dma((batches, GROUP)), dma((batches,)), dma((batches,)),
            dma((batches,)), dma((batches,)), dma((batches, 2)), dma((batches, 2)),
            dma((batches, CHUNKS)), dma((batches, CHUNKS)),
            dma((batches, CHUNKS)), dma((batches, CHUNKS)),
            dma((batches, 2, CHUNKS)), dma((batches, 2, CHUNKS)),
            dma((batches, 2, CHUNKS)), dma((batches, 2, CHUNKS)),
            dma((batches, CHUNKS)), dma((batches, CHUNKS)),
            dma((batches, n_seg)), dma((batches,)),
        ],
        compiler_params=pltpu.CompilerParams(
            collective_id=0, has_side_effects=True, vmem_limit_bytes=56 * 1024 * 1024
        ),
    )(src, tgt, slen, tlen, win, wout, gain, fgain.reshape(1, -1))


def solution(mesh):
    spec = P("dp", None, "segment")
    return jax.shard_map(
        functools.partial(on_device, mesh.shape["segment"], mesh.shape["dp"]),
        mesh=mesh,
        in_specs=(spec, spec, P("dp"), P("dp"), P("segment", None, None), P("segment", None, None), P(), P()),
        out_specs=spec,
        check_vma=False,
    )
```

```python
import functools

import jax
import jax.numpy as jnp
from jax import lax
from jax.experimental import pallas as pl
from jax.experimental.pallas import tpu as pltpu
from jax.sharding import PartitionSpec as P

HEAD = 64
GROUP = 4
CHUNKS = 4
AHEAD = 1
EARLY = 0
EPS = 1e-06
SCALE = 0.125
MASKED = -1000000000.0
MESH = pl.DeviceIdType.MESH
F32 = jnp.float32
BF16 = jnp.bfloat16


def rms(values, gain):
    return values * lax.rsqrt(jnp.mean(values * values, axis=-1, keepdims=True) + EPS) * gain


def kernel(
    n_seg, n_dp, src, tgt, slen, tlen, win, wout, gain, fgain, out,
    w_in, w_out, w_far, lens_own, lens_far, lens, arr, tg, nb, qs, acc, qkv, mix, mix_far, pf, part, rx, rz, zs, yb,
    go, wsem, lens_s, lens_r, far_s, far_r, mix_s, mix_r, src_s, tgt_s, src_r, tgt_r, tz_s, tz_r, tx_s, tx_r,
    relay_s, relay_r, agz_s, agz_r, agx_s, agx_r, rsx_s, rsx_r, rsz_s, rsz_r, out_s, out_r,
):
    batches, seq, cols = src.shape
    rows = seq // GROUP
    half = seq // 2
    block = cols * n_seg // CHUNKS
    heads = w_out.shape[0]
    s = lax.axis_index("segment")
    sect = s // GROUP
    m = s % GROUP
    zl = m // 2
    xl = m % 2
    x_near = s + 1 - 2 * xl
    d = lax.axis_index("dp")
    flipped = d + 2 - 4 * ((d // 2) % 2)
    alt = d % 2 == 1
    swap = alt & (xl == 1)
    x_dp = jnp.where(alt, flipped, d)
    work_dp = jnp.where(swap, flipped, d)
    core = d % 2
    twin = d + 1 - 2 * core
    own_q = xl * 2 + zl
    z_q = xl * 2 + 1 - zl
    lower = (sect > 0) & (zl == 0)
    upper = (sect > 0) & (zl == 1)
    z_near = s + 2 - 4 * zl
    last = n_seg // GROUP - 1

    load_in = pltpu.make_async_copy(win.at[0], w_in, wsem.at[0])
    load_out = pltpu.make_async_copy(wout.at[0], w_out, wsem.at[1])
    load_in.start()
    load_out.start()

    barrier = pltpu.get_barrier_semaphore()
    for k in range(1, n_seg):
        pl.semaphore_signal(
            barrier, inc=1, device_id={"segment": (s + k) % n_seg}, device_id_type=MESH
        )
    pl.semaphore_signal(
        barrier, inc=1, device_id={"segment": s, "dp": twin}, device_id_type=MESH
    )
    for k in range(1, n_dp // 4):
        pl.semaphore_signal(
            barrier, inc=1, device_id={"segment": s, "dp": (d + 4 * k) % n_dp}, device_id_type=MESH
        )

    @pl.when(alt)
    def _():
        for k in range(n_seg):
            pl.semaphore_signal(
                barrier, inc=1, device_id={"segment": k, "dp": flipped}, device_id_type=MESH
            )

    row = lax.broadcasted_iota(jnp.int32, lens_own.shape, 0)
    table = jnp.zeros(lens_own.shape, F32)
    for k in range(batches):
        table = jnp.where(row == k, slen[k].astype(F32), table)
        table = jnp.where(row == batches + k, tlen[k].astype(F32), table)
    lens_own[...] = table
    with jax.named_scope("barrier"):
        pl.semaphore_wait(barrier, n_seg + n_dp // 4 - 1 + jnp.where(alt, n_seg, 0))

    def remote(src_ref, dst_ref, send, recv, target, target_dp=None):
        return pltpu.make_async_remote_copy(
            src_ref=src_ref, dst_ref=dst_ref, send_sem=send, recv_sem=recv,
            device_id={"segment": target, "dp": d if target_dp is None else target_dp},
            device_id_type=MESH,
        )

    def lens_copy():
        return remote(lens_own, lens_far, lens_s, lens_r, s, flipped)

    @pl.when(swap)
    def _():
        lens_copy().start()

    def wait_for(ref, sem):
        pltpu.make_async_copy(ref, ref, sem).wait()

    def quarter(q):
        return pl.ds(pl.multiple_of(q * rows, rows), rows)

    def strip(c):
        return slice(c * block, (c + 1) * block)

    tall = n_dp // 4
    share = heads // (2 * tall)
    y = d // 4

    def far_rows(level):
        return pl.ds(pl.multiple_of((core * tall + level) * share, share), share)

    def far_copy():
        return remote(wout.at[0, far_rows(y)], w_far.at[far_rows(y)], far_s.at[0], far_r.at[0], z_near)

    def far_side(k):
        ref = w_far.at[far_rows(y)]
        return remote(ref, ref, far_s.at[k], far_r.at[k], s, (d + 4 * k) % n_dp)

    def far_swap():
        ref = w_far.at[pl.ds(pl.multiple_of(core * (heads // 2), heads // 2), heads // 2)]
        return remote(ref, ref, far_s.at[tall], far_r.at[tall], s, twin)

    own_cols = pl.ds(pl.multiple_of(s * cols, cols), cols)

    def part_of(t):
        return slice((t % 2 * 2 + t // 2) * rows, (t % 2 * 2 + t // 2 + 1) * rows)

    def spread(given, held, send, recv, first, b, t):
        return remote(
            given.at[b, part_of(t)], held.at[b, part_of(t), own_cols],
            send.at[b, t], recv.at[b], first + t,
            jnp.where(alt, flipped, d) if t % 2 == 1 else d,
        )

    def stays(first, t):
        same = s == first + t
        return same & jnp.logical_not(alt) if t % 2 == 1 else same

    def scatter(given, held, send, recv, first, b):
        for t in range(GROUP):
            @pl.when(jnp.logical_not(stays(first, t)))
            def _():
                spread(given, held, send, recv, first, b, t).start()

            @pl.when(stays(first, t))
            def _():
                pltpu.make_async_copy(
                    given.at[b, part_of(t)], held.at[b, part_of(t), own_cols], recv.at[b]
                ).start()

    def scattered(given, held, send, recv, first, b):
        for t in range(GROUP):
            @pl.when(jnp.logical_not(stays(first, t)))
            def _():
                spread(given, held, send, recv, first, b, t).wait_send()

    def give_source(b, carry):
        scatter(src, arr, src_s, src_r, 0, b)
        return carry

    @pl.when(lower & (sect == 1))
    def _():
        far_copy().start()

    give_source(0, 0)
    give_source(1, 0)

    def give_target(b, carry):
        scatter(tgt, tg, tgt_s, tgt_r, 2 * GROUP, b)
        return carry

    def paced(b, carry):
        give_source(b, carry)
        scattered(src, arr, src_s, src_r, 0, b)
        return carry

    @pl.when(sect == 0)
    def _():
        with jax.named_scope("first_wait"):
            wait_for(arr.at[0, quarter(own_q)], src_r.at[0])

    @pl.when(sect > 0)
    def _():
        scattered(src, arr, src_s, src_r, 0, 0)
        scattered(src, arr, src_s, src_r, 0, 1)
        lax.fori_loop(0, batches, give_target, 0)

    @pl.when(lower & (sect == 2))
    def _():
        far_copy().start()

    def far_share():
        with jax.named_scope("far"):
            far_copy().wait_recv()
            for k in range(1, tall):
                far_side(k).start()

    @pl.when(upper & (sect < last))
    def _():
        far_share()

    @pl.when(sect > 0)
    def _():
        with jax.named_scope("go_wait"):
            pl.semaphore_wait(go, GROUP)

    @pl.when(sect == 1)
    def _():
        lax.fori_loop(2, batches, give_source, 0)

    @pl.when(sect > 1)
    def _():
        with jax.named_scope("paced"):
            lax.fori_loop(2, batches, paced, 0)

    @pl.when(lower & (sect > 2))
    def _():
        far_copy().start()

    def go_ahead():
        for k in range(GROUP, n_seg):
            pl.semaphore_signal(
                go, inc=1, device_id={"segment": k, "dp": work_dp}, device_id_type=MESH
            )
        lax.fori_loop(2, batches, give_source, 0)

    def side_rows(side):
        return pl.ds(pl.multiple_of(side * half, half), half)

    def relay_first(b, c):
        return remote(
            yb.at[b, :rows, strip(c)], arr.at[b, quarter(own_q), strip(c)], relay_s.at[b, c],
            relay_r.at[b, c], GROUP + xl,
        )

    def relay(b, c):
        return remote(
            yb.at[b, :, strip(c)], arr.at[b, side_rows(xl), strip(c)],
            relay_s.at[b, c], relay_r.at[b, c], (s + 2) % n_seg,
        )

    def gather_z(b, c):
        ref = arr.at[b, quarter(own_q), strip(c)]
        return remote(ref, ref, agz_s.at[b, c], agz_r.at[b, c], z_near)

    def gather_x(b, which, c):
        ref = arr.at[b, quarter(own_q if which == 0 else z_q), strip(c)]
        return remote(ref, ref, agx_s.at[b, which, c], agx_r.at[b, which, c], x_near, x_dp)

    def lift_z(b, c):
        ref = arr.at[b, side_rows(xl), strip(c)]
        return remote(ref, ref, agz_s.at[b, c], agz_r.at[b, c], z_near)

    def half_x(b, c):
        ref = arr.at[b, side_rows(xl), strip(c)]
        return remote(ref, ref, agx_s.at[b, 0, c], agx_r.at[b, 0, c], x_near, x_dp)

    def mix_z(b):
        return remote(mix.at[b], mix_far.at[b], mix_s.at[b], mix_r.at[b], z_near)

    def target_z(b):
        ref = tg.at[b, quarter(own_q)]
        return remote(ref, ref, tz_s.at[b], tz_r.at[b], z_near)

    def target_x(b, which):
        ref = tg.at[b, quarter(own_q if which == 0 else z_q)]
        return remote(ref, ref, tx_s.at[b, which], tx_r.at[b, which], x_near, x_dp)

    def sum_x(b, which, c):
        wanted = (1 - xl) * 2 + (1 - zl if which == 0 else zl)
        return remote(
            part.at[b, quarter(wanted), strip(c)], rx.at[b, which * rows:(which + 1) * rows, strip(c)],
            rsx_s.at[b, which, c], rsx_r.at[b, which, c], x_near, x_dp,
        )

    def sum_half(b, c):
        return remote(
            part.at[b, side_rows(1 - xl), strip(c)], rx.at[b, :, strip(c)],
            rsx_s.at[b, 0, c], rsx_r.at[b, 0, c], x_near, x_dp,
        )

    def sum_z(b, c):
        return remote(zs.at[b, :, strip(c)], rz.at[b, :, strip(c)], rsz_s.at[b, c], rsz_r.at[b, c], z_near)

    def out_copy(b, t):
        return remote(
            yb.at[b, :, pl.ds(pl.multiple_of(t * cols, cols), cols)],
            out.at[b, pl.ds(pl.multiple_of(xl * half, half), half)], out_s.at[b, t], out_r.at[b], t, work_dp,
        )

    def step_r(b, waits=True):
        if waits:
            with jax.named_scope("r_wait"):
                wait_for(arr.at[b, quarter(own_q)], src_r.at[b])
        for c in range(CHUNKS):
            gather_z(b, c).start()
            gather_x(b, 0, c).start()

    def step_f(b, c):
        with jax.named_scope("f_wait"):
            gather_z(b, c).wait_recv()
        gather_x(b, 1, c).start()

    def step_r2(b, c):
        with jax.named_scope("r_wait"):
            wait_for(arr.at[b, side_rows(xl), strip(c)], relay_r.at[b, c])
        lift_z(b, c).start()
        half_x(b, c).start()

    def step_f2(b, c):
        with jax.named_scope("f_wait"):
            lift_z(b, c).wait_recv()
        half_x(b, c).start()

    own_gain = gain[pl.ds(sect, 1), :]

    strip_gain = jnp.where(sect == 2, fgain[...], own_gain)

    def project(b, wait):
        squares = jnp.zeros((seq, 1), F32)
        for c in range(CHUNKS):
            wait(c)
            held = arr[b, :, strip(c)].astype(F32)
            squares = squares + jnp.sum(held * held, axis=-1, keepdims=True)
            nb[:, strip(c)] = (held * strip_gain[:, strip(c)]).astype(BF16)
            with jax.named_scope("kv_dot"):
                grown = jnp.dot(nb[:, strip(c)], w_in[strip(c), :], preferred_element_type=F32)
                if c == 0:
                    acc[...] = grown
                elif c < CHUNKS - 1:
                    acc[...] += grown
                else:
                    scale = lax.rsqrt(squares / (cols * n_seg) + EPS)
                    qkv[...] = ((acc[...] + grown) * scale).astype(BF16)

        @pl.when(sect == 2)
        def _():
            qkv[:, :heads] = qs[b]

    def attend(b):
        length = lens[pl.ds(jnp.where(sect == last, batches, 0) + b, 1), :seq]
        query_pos = lax.broadcasted_iota(jnp.int32, (seq, seq), 0)
        key_pos = lax.broadcasted_iota(jnp.int32, (seq, seq), 1)
        limit = jnp.where(sect == last, query_pos, seq)
        allowed = (key_pos.astype(F32) < length) & (key_pos <= limit)
        allowed = jnp.concatenate([allowed, allowed], axis=0)
        pair = 2 * HEAD
        low = lax.broadcasted_iota(jnp.int32, (seq, pair), 1) < HEAD
        for j in range(heads // pair):
            q2 = qkv[:, j * pair:(j + 1) * pair]
            k2 = qkv[:, heads + j * pair:heads + (j + 1) * pair]
            v2 = qkv[:, 2 * heads + j * pair:2 * heads + (j + 1) * pair]
            zero = jnp.zeros_like(q2)
            stacked = jnp.concatenate([jnp.where(low, q2, zero), jnp.where(low, zero, q2)], axis=0)
            scores = lax.dot_general(
                stacked, k2, (((1,), (1,)), ((), ())), preferred_element_type=F32
            ) * SCALE
            scores = jnp.where(allowed, scores, MASKED)
            grown = jnp.exp(scores - jnp.max(scores, axis=-1, keepdims=True))
            weights = (grown / jnp.sum(grown, axis=-1, keepdims=True)).astype(BF16)
            both = jnp.dot(weights, v2, preferred_element_type=F32)
            mix[b, :, j * pair:(j + 1) * pair] = jnp.where(low, both[:seq], both[seq:]).astype(BF16)

    def step_z(b, c):
        with jax.named_scope("z_wait"):
            sum_x(b, 0, c).wait_recv()
        zs[b, :, strip(c)] = (pf[quarter(z_q), strip(c)] + rx[b, :rows, strip(c)].astype(F32)).astype(BF16)
        sum_z(b, c).start()

    def step_y(b, c):
        with jax.named_scope("y_wait"):
            sum_x(b, 1, c).wait_recv()
            sum_z(b, c).wait_recv()
        total = (
            pf[quarter(own_q), strip(c)] + rx[b, rows:, strip(c)].astype(F32)
            + rz[b, :, strip(c)].astype(F32)
        )
        yb[b, :rows, strip(c)] = (arr[b, quarter(own_q), strip(c)].astype(F32) + total).astype(BF16)
        relay_first(b, c).start()

    def step_y2(b, c):
        with jax.named_scope("y_wait"):
            sum_half(b, c).wait_recv()
        mine = side_rows(xl)
        total = pf[mine, strip(c)] + rx[b, :, strip(c)].astype(F32)

        @pl.when(sect == 2)
        def _():
            yb[b, :, strip(c)] = (tg[b, mine, strip(c)].astype(F32) + total).astype(BF16)

        @pl.when(sect != 2)
        def _():
            yb[b, :, strip(c)] = (arr[b, mine, strip(c)].astype(F32) + total).astype(BF16)

        @pl.when(sect < last)
        def _():
            relay(b, c).start()

        if c == CHUNKS - 1:
            @pl.when(sect == last)
            def _():
                def one(t, carry):
                    @pl.when((t != s) | swap)
                    def _():
                        out_copy(b, t).start()

                    @pl.when((t == s) & jnp.logical_not(swap))
                    def _():
                        pltpu.make_async_copy(
                            yb.at[b, :, own_cols],
                            out.at[b, pl.ds(pl.multiple_of(xl * half, half), half)], out_r.at[b],
                        ).start()
                    return carry

                lax.fori_loop(0, n_seg, one, 0)

    @pl.when(swap)
    def _():
        lens_copy().wait()
        lens[...] = lens_far[...]

    @pl.when(jnp.logical_not(swap))
    def _():
        lens[...] = lens_own[...]

    with jax.named_scope("load"):
        load_in.wait()
        load_out.wait()

    @pl.when(sect == 2)
    def _():
        def first(b, carry):
            wait_for(tg.at[b, quarter(own_q)], tgt_r.at[b])
            target_z(b).start()
            target_x(b, 0).start()
            return carry

        lax.fori_loop(0, batches, first, 0)

    @pl.when(upper & (sect == last))
    def _():
        far_share()

    @pl.when(sect == 2)
    def _():
        def second(b, carry):
            target_z(b).wait_recv()
            target_x(b, 1).start()
            return carry

        lax.fori_loop(0, batches, second, 0)

        def third(b, carry):
            target_x(b, 0).wait_recv()
            target_x(b, 1).wait_recv()
            nb[...] = rms(tg[b].astype(F32), own_gain).astype(BF16)
            qs[b] = jnp.dot(nb[...], w_in[:, :heads], preferred_element_type=F32).astype(BF16)
            return carry

        with jax.named_scope("target_q"):
            lax.fori_loop(0, batches, third, 0)

    @pl.when(upper)
    def _():
        with jax.named_scope("far_side"):
            for k in range(1, tall):
                wait_for(w_far.at[far_rows((y + tall - k) % tall)], far_r.at[k])
            far_swap().start()

    @pl.when(sect == 0)
    def _():
        step_r(0, False)
        lax.fori_loop(0, batches, give_target, 0)
        for c in range(CHUNKS):
            step_f(0, c)
        step_r(1)

    @pl.when(upper)
    def _():
        for c in range(CHUNKS):
            step_f2(0, c)
        far_swap().wait_recv()

    def main(b, carry):
        more = b < batches - 1

        @pl.when(lower)
        def _():
            for c in range(CHUNKS):
                step_r2(b, c)

        @pl.when(more & (sect == 0) & (b > 0))
        def _():
            step_r(b + 1)

        def arrived(c):
            with jax.named_scope("c_wait"):
                @pl.when(sect == 0)
                def _():
                    gather_x(b, 0, c).wait_recv()
                    gather_x(b, 1, c).wait_recv()

                @pl.when(sect > 0)
                def _():
                    half_x(b, c).wait_recv()

        project(b, arrived)

        @pl.when((sect == 0) & (b == 0))
        def _():
            go_ahead()
        attend(b)

        @pl.when(lower)
        def _():
            mix_z(b).start()

        @pl.when(sect == 0)
        def _():
            for c in range(CHUNKS):
                with jax.named_scope("out_dot"):
                    total = jnp.dot(mix[b], w_out[:, strip(c)], preferred_element_type=F32)
                    pf[:, strip(c)] = total
                    part[b, :, strip(c)] = total.astype(BF16)
                sum_x(b, 0, c).start()
            for c in range(CHUNKS):
                sum_x(b, 1, c).start()

            @pl.when(more)
            def _():
                for c in range(CHUNKS):
                    step_f(b + 1, c)

            for c in range(CHUNKS):
                step_z(b, c)
            for c in range(CHUNKS):
                step_y(b, c)

        @pl.when(upper)
        def _():
            @pl.when(more)
            def _():
                for c in range(EARLY):
                    step_f2(b + 1, c)

            with jax.named_scope("mix_wait"):
                mix_z(b).wait_recv()
            for c in range(CHUNKS):
                with jax.named_scope("out_dot2"):
                    total = jnp.dot(mix[b], w_out[:, strip(c)], preferred_element_type=F32)
                    total = total + jnp.dot(mix_far[b], w_far[:, strip(c)], preferred_element_type=F32)
                    pf[:, strip(c)] = total
                    part[b, :, strip(c)] = total.astype(BF16)
                sum_half(b, c).start()

            @pl.when(b == 0)
            def _():
                for c in range(CHUNKS):
                    step_y2(b, c)
                    if c > 0:
                        step_f2(b + 1, c - 1)
                step_f2(b + 1, CHUNKS - 1)

            @pl.when(b > 0)
            def _():
                for c in range(CHUNKS):
                    @pl.when(more)
                    def _():
                        step_f2(b + 1, c)

                    step_y2(b, c)
        return carry

    lax.fori_loop(0, batches, main, 0)

    def finish(b, carry):
        @pl.when((sect == 0) | ((sect == 1) & (b > 1)))
        def _():
            scattered(src, arr, src_s, src_r, 0, b)

        scattered(tgt, tg, tgt_s, tgt_r, 2 * GROUP, b)
        for c in range(CHUNKS):
            @pl.when(sect == 0)
            def _():
                sum_x(b, 0, c).wait_send()
                sum_x(b, 1, c).wait_send()
                sum_z(b, c).wait_send()
                gather_z(b, c).wait_send()
                gather_x(b, 0, c).wait_send()
                gather_x(b, 1, c).wait_send()
                relay_first(b, c).wait_send()

            @pl.when(lower)
            def _():
                lift_z(b, c).wait_send()
                half_x(b, c).wait_send()

            @pl.when(upper)
            def _():
                half_x(b, c).wait_send()
                sum_half(b, c).wait_send()

            @pl.when(upper & (sect < last))
            def _():
                relay(b, c).wait_send()

        @pl.when(lower)
        def _():
            mix_z(b).wait_send()

        @pl.when(sect == 2)
        def _():
            target_z(b).wait_send()
            target_x(b, 0).wait_send()
            target_x(b, 1).wait_send()

        @pl.when(upper & (sect == last))
        def _():
            def one(t, inner):
                @pl.when((t != s) | swap)
                def _():
                    out_copy(b, t).wait_send()
                return inner

            lax.fori_loop(0, n_seg, one, 0)

        with jax.named_scope("o_wait"):
            wait_for(out.at[b], out_r.at[b])
        return carry

    lax.fori_loop(0, batches, finish, 0)

    @pl.when(lower)
    def _():
        far_copy().wait_send()

    @pl.when(upper)
    def _():
        far_swap().wait_send()
        for k in range(1, tall):
            far_side(k).wait_send()


def on_device(n_seg, n_dp, src, tgt, slen, tlen, win, wout, gain, fgain):
    batches, seq, cols = src.shape
    width = cols * n_seg
    depth, fan = win.shape[1:]
    heads = wout.shape[1]
    rows = seq // GROUP
    any_space = pl.BlockSpec(memory_space=pl.ANY)
    vmem = pl.BlockSpec(memory_space=pltpu.VMEM)
    smem = pl.BlockSpec(memory_space=pltpu.SMEM)
    dma = pltpu.SemaphoreType.DMA
    return pl.pallas_call(
        functools.partial(kernel, n_seg, n_dp),
        out_shape=jax.ShapeDtypeStruct((batches, seq, cols), BF16),
        in_specs=[any_space, any_space, smem, smem, any_space, any_space, vmem, vmem],
        out_specs=any_space,
        scratch_shapes=[
            pltpu.VMEM((depth, fan), BF16),
            pltpu.VMEM((heads, width), BF16),
            pltpu.VMEM((heads, width), BF16),
            pltpu.VMEM((2 * batches, 128), F32),
            pltpu.VMEM((2 * batches, 128), F32),
            pltpu.VMEM((2 * batches, 128), F32),
            pltpu.VMEM((batches, seq, width), BF16),
            pltpu.VMEM((batches, seq, width), BF16),
            pltpu.VMEM((seq, width), BF16),
            pltpu.VMEM((batches, seq, heads), BF16),
            pltpu.VMEM((seq, fan), F32),
            pltpu.VMEM((seq, fan), BF16),
            pltpu.VMEM((batches, seq, heads), BF16),
            pltpu.VMEM((batches, seq, heads), BF16),
            pltpu.VMEM((seq, width), F32),
            pltpu.VMEM((batches, seq, width), BF16),
            pltpu.VMEM((batches, 2 * rows, width), BF16),
            pltpu.VMEM((batches, rows, width), BF16),
            pltpu.VMEM((batches, rows, width), BF16),
            pltpu.VMEM((batches, 2 * rows, width), BF16),
            pltpu.SemaphoreType.REGULAR, dma((2,)), dma, dma, dma((n_dp // 4 + 1,)), dma((n_dp // 4 + 1,)), dma((batches,)), dma((batches,)),
            dma((batches, GROUP)), dma((batches, GROUP)), dma((batches,)), dma((batches,)),
            dma((batches,)), dma((batches,)), dma((batches, 2)), dma((batches, 2)),
            dma((batches, CHUNKS)), dma((batches, CHUNKS)),
            dma((batches, CHUNKS)), dma((batches, CHUNKS)),
            dma((batches, 2, CHUNKS)), dma((batches, 2, CHUNKS)),
            dma((batches, 2, CHUNKS)), dma((batches, 2, CHUNKS)),
            dma((batches, CHUNKS)), dma((batches, CHUNKS)),
            dma((batches, n_seg)), dma((batches,)),
        ],
        compiler_params=pltpu.CompilerParams(
            collective_id=0, has_side_effects=True, vmem_limit_bytes=56 * 1024 * 1024
        ),
    )(src, tgt, slen, tlen, win, wout, gain, fgain.reshape(1, -1))


def solution(mesh):
    spec = P("dp", None, "segment")
    return jax.shard_map(
        functools.partial(on_device, mesh.shape["segment"], mesh.shape["dp"]),
        mesh=mesh,
        in_specs=(spec, spec, P("dp"), P("dp"), P("segment", None, None), P("segment", None, None), P(), P()),
        out_specs=spec,
        check_vma=False,
    )
```

```python
import functools

import jax
import jax.numpy as jnp
from jax import lax
from jax.experimental import pallas as pl
from jax.experimental.pallas import tpu as pltpu
from jax.sharding import PartitionSpec as P

HEAD = 64
GROUP = 4
CHUNKS = 8
AHEAD = 1
EARLY = 0
EPS = 1e-06
SCALE = 0.125
MASKED = -1000000000.0
MESH = pl.DeviceIdType.MESH
F32 = jnp.float32
BF16 = jnp.bfloat16


def rms(values, gain):
    return values * lax.rsqrt(jnp.mean(values * values, axis=-1, keepdims=True) + EPS) * gain


def kernel(
    n_seg, n_dp, src, tgt, slen, tlen, win, wout, gain, fgain, out,
    w_in, w_out, w_far, lens_own, lens_far, lens, arr, tg, nb, qs, acc, qkv, mix, mix_far, pf, part, rx, rz, zs, yb,
    go, wsem, lens_s, lens_r, far_s, far_r, mix_s, mix_r, src_s, tgt_s, src_r, tgt_r, tz_s, tz_r, tx_s, tx_r,
    relay_s, relay_r, agz_s, agz_r, agx_s, agx_r, rsx_s, rsx_r, rsz_s, rsz_r, out_s, out_r,
):
    batches, seq, cols = src.shape
    rows = seq // GROUP
    half = seq // 2
    block = cols * n_seg // CHUNKS
    heads = w_out.shape[0]
    s = lax.axis_index("segment")
    sect = s // GROUP
    m = s % GROUP
    zl = m // 2
    xl = m % 2
    x_near = s + 1 - 2 * xl
    d = lax.axis_index("dp")
    flipped = d + 2 - 4 * ((d // 2) % 2)
    alt = d % 2 == 1
    swap = alt & (xl == 1)
    x_dp = jnp.where(alt, flipped, d)
    work_dp = jnp.where(swap, flipped, d)
    core = d % 2
    twin = d + 1 - 2 * core
    own_q = xl * 2 + zl
    z_q = xl * 2 + 1 - zl
    lower = (sect > 0) & (zl == 0)
    upper = (sect > 0) & (zl == 1)
    z_near = s + 2 - 4 * zl
    last = n_seg // GROUP - 1

    load_in = pltpu.make_async_copy(win.at[0], w_in, wsem.at[0])
    load_out = pltpu.make_async_copy(wout.at[0], w_out, wsem.at[1])
    load_in.start()
    load_out.start()

    barrier = pltpu.get_barrier_semaphore()
    for k in range(1, n_seg):
        pl.semaphore_signal(
            barrier, inc=1, device_id={"segment": (s + k) % n_seg}, device_id_type=MESH
        )
    pl.semaphore_signal(
        barrier, inc=1, device_id={"segment": s, "dp": twin}, device_id_type=MESH
    )
    for k in range(1, n_dp // 4):
        pl.semaphore_signal(
            barrier, inc=1, device_id={"segment": s, "dp": (d + 4 * k) % n_dp}, device_id_type=MESH
        )

    @pl.when(alt)
    def _():
        for k in range(n_seg):
            pl.semaphore_signal(
                barrier, inc=1, device_id={"segment": k, "dp": flipped}, device_id_type=MESH
            )

    row = lax.broadcasted_iota(jnp.int32, lens_own.shape, 0)
    table = jnp.zeros(lens_own.shape, F32)
    for k in range(batches):
        table = jnp.where(row == k, slen[k].astype(F32), table)
        table = jnp.where(row == batches + k, tlen[k].astype(F32), table)
    lens_own[...] = table
    with jax.named_scope("barrier"):
        pl.semaphore_wait(barrier, n_seg + n_dp // 4 - 1 + jnp.where(alt, n_seg, 0))

    def remote(src_ref, dst_ref, send, recv, target, target_dp=None):
        return pltpu.make_async_remote_copy(
            src_ref=src_ref, dst_ref=dst_ref, send_sem=send, recv_sem=recv,
            device_id={"segment": target, "dp": d if target_dp is None else target_dp},
            device_id_type=MESH,
        )

    def lens_copy():
        return remote(lens_own, lens_far, lens_s, lens_r, s, flipped)

    @pl.when(swap)
    def _():
        lens_copy().start()

    def wait_for(ref, sem):
        pltpu.make_async_copy(ref, ref, sem).wait()

    def quarter(q):
        return pl.ds(pl.multiple_of(q * rows, rows), rows)

    def strip(c):
        return slice(c * block, (c + 1) * block)

    tall = n_dp // 4
    share = heads // (2 * tall)
    y = d // 4

    def far_rows(level):
        return pl.ds(pl.multiple_of((core * tall + level) * share, share), share)

    def far_copy():
        return remote(wout.at[0, far_rows(y)], w_far.at[far_rows(y)], far_s.at[0], far_r.at[0], z_near)

    def far_side(k):
        ref = w_far.at[far_rows(y)]
        return remote(ref, ref, far_s.at[k], far_r.at[k], s, (d + 4 * k) % n_dp)

    def far_swap():
        ref = w_far.at[pl.ds(pl.multiple_of(core * (heads // 2), heads // 2), heads // 2)]
        return remote(ref, ref, far_s.at[tall], far_r.at[tall], s, twin)

    own_cols = pl.ds(pl.multiple_of(s * cols, cols), cols)

    def part_of(t):
        return slice((t % 2 * 2 + t // 2) * rows, (t % 2 * 2 + t // 2 + 1) * rows)

    def spread(given, held, send, recv, first, b, t):
        return remote(
            given.at[b, part_of(t)], held.at[b, part_of(t), own_cols],
            send.at[b, t], recv.at[b], first + t,
            jnp.where(alt, flipped, d) if t % 2 == 1 else d,
        )

    def stays(first, t):
        same = s == first + t
        return same & jnp.logical_not(alt) if t % 2 == 1 else same

    def scatter(given, held, send, recv, first, b):
        for t in range(GROUP):
            @pl.when(jnp.logical_not(stays(first, t)))
            def _():
                spread(given, held, send, recv, first, b, t).start()

            @pl.when(stays(first, t))
            def _():
                pltpu.make_async_copy(
                    given.at[b, part_of(t)], held.at[b, part_of(t), own_cols], recv.at[b]
                ).start()

    def scattered(given, held, send, recv, first, b):
        for t in range(GROUP):
            @pl.when(jnp.logical_not(stays(first, t)))
            def _():
                spread(given, held, send, recv, first, b, t).wait_send()

    def give_source(b, carry):
        scatter(src, arr, src_s, src_r, 0, b)
        return carry

    @pl.when(lower & (sect == 1))
    def _():
        far_copy().start()

    give_source(0, 0)
    give_source(1, 0)

    def give_target(b, carry):
        scatter(tgt, tg, tgt_s, tgt_r, 2 * GROUP, b)
        return carry

    def paced(b, carry):
        give_source(b, carry)
        scattered(src, arr, src_s, src_r, 0, b)
        return carry

    @pl.when(sect == 0)
    def _():
        with jax.named_scope("first_wait"):
            wait_for(arr.at[0, quarter(own_q)], src_r.at[0])

    @pl.when(sect > 0)
    def _():
        scattered(src, arr, src_s, src_r, 0, 0)
        scattered(src, arr, src_s, src_r, 0, 1)
        lax.fori_loop(0, batches, give_target, 0)

    @pl.when(lower & (sect == 2))
    def _():
        far_copy().start()

    def far_share():
        with jax.named_scope("far"):
            far_copy().wait_recv()
            for k in range(1, tall):
                far_side(k).start()

    @pl.when(upper & (sect < last))
    def _():
        far_share()

    @pl.when(sect > 0)
    def _():
        with jax.named_scope("go_wait"):
            pl.semaphore_wait(go, GROUP)

    @pl.when(sect == 1)
    def _():
        lax.fori_loop(2, batches, give_source, 0)

    @pl.when(sect > 1)
    def _():
        with jax.named_scope("paced"):
            lax.fori_loop(2, batches, paced, 0)

    @pl.when(lower & (sect > 2))
    def _():
        far_copy().start()

    def go_ahead():
        for k in range(GROUP, n_seg):
            pl.semaphore_signal(
                go, inc=1, device_id={"segment": k, "dp": work_dp}, device_id_type=MESH
            )
        lax.fori_loop(2, batches, give_source, 0)

    def side_rows(side):
        return pl.ds(pl.multiple_of(side * half, half), half)

    def relay_first(b, c):
        return remote(
            yb.at[b, :rows, strip(c)], arr.at[b, quarter(own_q), strip(c)], relay_s.at[b, c],
            relay_r.at[b, c], GROUP + xl,
        )

    def relay(b, c):
        return remote(
            yb.at[b, :, strip(c)], arr.at[b, side_rows(xl), strip(c)],
            relay_s.at[b, c], relay_r.at[b, c], (s + 2) % n_seg,
        )

    def gather_z(b, c):
        ref = arr.at[b, quarter(own_q), strip(c)]
        return remote(ref, ref, agz_s.at[b, c], agz_r.at[b, c], z_near)

    def gather_x(b, which, c):
        ref = arr.at[b, quarter(own_q if which == 0 else z_q), strip(c)]
        return remote(ref, ref, agx_s.at[b, which, c], agx_r.at[b, which, c], x_near, x_dp)

    def lift_z(b, c):
        ref = arr.at[b, side_rows(xl), strip(c)]
        return remote(ref, ref, agz_s.at[b, c], agz_r.at[b, c], z_near)

    def half_x(b, c):
        ref = arr.at[b, side_rows(xl), strip(c)]
        return remote(ref, ref, agx_s.at[b, 0, c], agx_r.at[b, 0, c], x_near, x_dp)

    def mix_z(b, k):
        side = slice(k * heads // 2, (k + 1) * heads // 2)
        return remote(
            mix.at[b, :, side], mix_far.at[b, :, side], mix_s.at[b, k], mix_r.at[b, k], z_near
        )

    def target_z(b):
        ref = tg.at[b, quarter(own_q)]
        return remote(ref, ref, tz_s.at[b], tz_r.at[b], z_near)

    def target_x(b, which):
        ref = tg.at[b, quarter(own_q if which == 0 else z_q)]
        return remote(ref, ref, tx_s.at[b, which], tx_r.at[b, which], x_near, x_dp)

    def sum_x(b, which, c):
        wanted = (1 - xl) * 2 + (1 - zl if which == 0 else zl)
        return remote(
            part.at[b, quarter(wanted), strip(c)], rx.at[b, which * rows:(which + 1) * rows, strip(c)],
            rsx_s.at[b, which, c], rsx_r.at[b, which, c], x_near, x_dp,
        )

    def sum_half(b, c):
        return remote(
            part.at[b, side_rows(1 - xl), strip(c)], rx.at[b, :, strip(c)],
            rsx_s.at[b, 0, c], rsx_r.at[b, 0, c], x_near, x_dp,
        )

    def sum_z(b, c):
        return remote(zs.at[b, :, strip(c)], rz.at[b, :, strip(c)], rsz_s.at[b, c], rsz_r.at[b, c], z_near)

    def out_copy(b, t):
        return remote(
            yb.at[b, :, pl.ds(t * cols if isinstance(t, int) else pl.multiple_of(t * cols, cols), cols)],
            out.at[b, pl.ds(pl.multiple_of(xl * half, half), half)], out_s.at[b, t], out_r.at[b], t, work_dp,
        )

    def step_r(b, waits=True):
        if waits:
            with jax.named_scope("r_wait"):
                wait_for(arr.at[b, quarter(own_q)], src_r.at[b])
        for c in range(CHUNKS):
            gather_z(b, c).start()
            gather_x(b, 0, c).start()

    def step_f(b, c):
        with jax.named_scope("f_wait"):
            gather_z(b, c).wait_recv()
        gather_x(b, 1, c).start()

    def step_r2(b, c):
        with jax.named_scope("r_wait"):
            wait_for(arr.at[b, side_rows(xl), strip(c)], relay_r.at[b, c])
        lift_z(b, c).start()
        half_x(b, c).start()

    def step_f2(b, c):
        with jax.named_scope("f_wait"):
            lift_z(b, c).wait_recv()
        half_x(b, c).start()

    own_gain = gain[pl.ds(sect, 1), :]

    strip_gain = jnp.where(sect == 2, fgain[...], own_gain)

    def project(b, wait):
        squares = jnp.zeros((seq, 1), F32)
        for c in range(CHUNKS):
            wait(c)
            held = arr[b, :, strip(c)].astype(F32)
            squares = squares + jnp.sum(held * held, axis=-1, keepdims=True)
            nb[:, strip(c)] = (held * strip_gain[:, strip(c)]).astype(BF16)
            with jax.named_scope("kv_dot"):
                grown = jnp.dot(nb[:, strip(c)], w_in[strip(c), :], preferred_element_type=F32)
                if c == 0:
                    acc[...] = grown
                elif c < CHUNKS - 1:
                    acc[...] += grown
                else:
                    scale = lax.rsqrt(squares / (cols * n_seg) + EPS)
                    qkv[...] = ((acc[...] + grown) * scale).astype(BF16)

        @pl.when(sect == 2)
        def _():
            qkv[:, :heads] = qs[b]

    def attend(b):
        length = lens[pl.ds(jnp.where(sect == last, batches, 0) + b, 1), :seq]
        query_pos = lax.broadcasted_iota(jnp.int32, (seq, seq), 0)
        key_pos = lax.broadcasted_iota(jnp.int32, (seq, seq), 1)
        limit = jnp.where(sect == last, query_pos, seq)
        allowed = (key_pos.astype(F32) < length) & (key_pos <= limit)
        allowed = jnp.concatenate([allowed, allowed], axis=0)
        pair = 2 * HEAD
        low = lax.broadcasted_iota(jnp.int32, (seq, pair), 1) < HEAD
        for j in range(heads // pair):
            q2 = qkv[:, j * pair:(j + 1) * pair]
            k2 = qkv[:, heads + j * pair:heads + (j + 1) * pair]
            v2 = qkv[:, 2 * heads + j * pair:2 * heads + (j + 1) * pair]
            zero = jnp.zeros_like(q2)
            stacked = jnp.concatenate([jnp.where(low, q2, zero), jnp.where(low, zero, q2)], axis=0)
            scores = lax.dot_general(
                stacked, k2, (((1,), (1,)), ((), ())), preferred_element_type=F32
            ) * SCALE
            scores = jnp.where(allowed, scores, MASKED)
            grown = jnp.exp(scores - jnp.max(scores, axis=-1, keepdims=True))
            weights = (grown / jnp.sum(grown, axis=-1, keepdims=True)).astype(BF16)
            both = jnp.dot(weights, v2, preferred_element_type=F32)
            mix[b, :, j * pair:(j + 1) * pair] = jnp.where(low, both[:seq], both[seq:]).astype(BF16)
            if (j + 1) * pair * 2 == heads:
                @pl.when(lower)
                def _():
                    mix_z(b, 0).start()

    def step_z(b, c):
        with jax.named_scope("z_wait"):
            sum_x(b, 0, c).wait_recv()
        zs[b, :, strip(c)] = (pf[quarter(z_q), strip(c)] + rx[b, :rows, strip(c)].astype(F32)).astype(BF16)
        sum_z(b, c).start()

    def step_y(b, c):
        with jax.named_scope("y_wait"):
            sum_x(b, 1, c).wait_recv()
            sum_z(b, c).wait_recv()
        total = (
            pf[quarter(own_q), strip(c)] + rx[b, rows:, strip(c)].astype(F32)
            + rz[b, :, strip(c)].astype(F32)
        )
        yb[b, :rows, strip(c)] = (arr[b, quarter(own_q), strip(c)].astype(F32) + total).astype(BF16)
        relay_first(b, c).start()

    def step_y2(b, c):
        with jax.named_scope("y_wait"):
            sum_half(b, c).wait_recv()
        mine = side_rows(xl)
        total = pf[mine, strip(c)] + rx[b, :, strip(c)].astype(F32)

        @pl.when(sect == 2)
        def _():
            yb[b, :, strip(c)] = (tg[b, mine, strip(c)].astype(F32) + total).astype(BF16)

        @pl.when(sect != 2)
        def _():
            yb[b, :, strip(c)] = (arr[b, mine, strip(c)].astype(F32) + total).astype(BF16)

        @pl.when(sect < last)
        def _():
            relay(b, c).start()

        @pl.when(sect == last)
        def _():
            for t in range(c * n_seg // CHUNKS, (c + 1) * n_seg // CHUNKS):
                @pl.when((t != s) | swap)
                def _():
                    out_copy(b, t).start()

                @pl.when((t == s) & jnp.logical_not(swap))
                def _():
                    pltpu.make_async_copy(
                        yb.at[b, :, own_cols],
                        out.at[b, pl.ds(pl.multiple_of(xl * half, half), half)], out_r.at[b],
                    ).start()

    @pl.when(swap)
    def _():
        lens_copy().wait()
        lens[...] = lens_far[...]

    @pl.when(jnp.logical_not(swap))
    def _():
        lens[...] = lens_own[...]

    with jax.named_scope("load"):
        load_in.wait()
        load_out.wait()

    @pl.when(sect == 2)
    def _():
        def first(b, carry):
            wait_for(tg.at[b, quarter(own_q)], tgt_r.at[b])
            target_z(b).start()
            target_x(b, 0).start()
            return carry

        lax.fori_loop(0, batches, first, 0)

    @pl.when(upper & (sect == last))
    def _():
        far_share()

    @pl.when(sect == 2)
    def _():
        def second(b, carry):
            target_z(b).wait_recv()
            target_x(b, 1).start()
            return carry

        lax.fori_loop(0, batches, second, 0)

        def third(b, carry):
            target_x(b, 0).wait_recv()
            target_x(b, 1).wait_recv()
            nb[...] = rms(tg[b].astype(F32), own_gain).astype(BF16)
            qs[b] = jnp.dot(nb[...], w_in[:, :heads], preferred_element_type=F32).astype(BF16)
            return carry

        with jax.named_scope("target_q"):
            lax.fori_loop(0, batches, third, 0)

    @pl.when(upper)
    def _():
        with jax.named_scope("far_side"):
            for k in range(1, tall):
                wait_for(w_far.at[far_rows((y + tall - k) % tall)], far_r.at[k])
            far_swap().start()

    @pl.when(sect == 0)
    def _():
        step_r(0, False)
        lax.fori_loop(0, batches, give_target, 0)
        for c in range(CHUNKS):
            step_f(0, c)
        step_r(1)

    @pl.when(upper)
    def _():
        for c in range(CHUNKS):
            step_f2(0, c)
        far_swap().wait_recv()

    def main(b, carry):
        more = b < batches - 1

        @pl.when(lower)
        def _():
            for c in range(CHUNKS):
                step_r2(b, c)

        @pl.when(more & (sect == 0) & (b > 0))
        def _():
            step_r(b + 1)

        def arrived(c):
            with jax.named_scope("c_wait"):
                @pl.when(sect == 0)
                def _():
                    gather_x(b, 0, c).wait_recv()
                    gather_x(b, 1, c).wait_recv()

                @pl.when(sect > 0)
                def _():
                    half_x(b, c).wait_recv()

        project(b, arrived)

        @pl.when((sect == 0) & (b == 0))
        def _():
            go_ahead()
        attend(b)

        @pl.when(lower)
        def _():
            mix_z(b, 1).start()

        @pl.when(sect == 0)
        def _():
            for c in range(CHUNKS):
                with jax.named_scope("out_dot"):
                    total = jnp.dot(mix[b], w_out[:, strip(c)], preferred_element_type=F32)
                    pf[:, strip(c)] = total
                    part[b, :, strip(c)] = total.astype(BF16)
                sum_x(b, 0, c).start()
            for c in range(CHUNKS):
                sum_x(b, 1, c).start()

            @pl.when(more)
            def _():
                for c in range(CHUNKS):
                    step_f(b + 1, c)

            for c in range(CHUNKS):
                step_z(b, c)
            for c in range(CHUNKS):
                step_y(b, c)

        @pl.when(upper)
        def _():
            @pl.when(more)
            def _():
                for c in range(EARLY):
                    step_f2(b + 1, c)

            with jax.named_scope("mix_wait"):
                mix_z(b, 0).wait_recv()
                mix_z(b, 1).wait_recv()
            for c in range(CHUNKS):
                with jax.named_scope("out_dot2"):
                    total = jnp.dot(mix[b], w_out[:, strip(c)], preferred_element_type=F32)
                    total = total + jnp.dot(mix_far[b], w_far[:, strip(c)], preferred_element_type=F32)
                    pf[:, strip(c)] = total
                    part[b, :, strip(c)] = total.astype(BF16)
                sum_half(b, c).start()

            @pl.when(b == 0)
            def _():
                for c in range(CHUNKS):
                    step_y2(b, c)
                    if c > 0:
                        step_f2(b + 1, c - 1)
                step_f2(b + 1, CHUNKS - 1)

            @pl.when(b > 0)
            def _():
                for c in range(CHUNKS):
                    @pl.when(more)
                    def _():
                        step_f2(b + 1, c)

                    step_y2(b, c)
        return carry

    lax.fori_loop(0, batches, main, 0)

    def finish(b, carry):
        @pl.when((sect == 0) | ((sect == 1) & (b > 1)))
        def _():
            scattered(src, arr, src_s, src_r, 0, b)

        scattered(tgt, tg, tgt_s, tgt_r, 2 * GROUP, b)
        for c in range(CHUNKS):
            @pl.when(sect == 0)
            def _():
                sum_x(b, 0, c).wait_send()
                sum_x(b, 1, c).wait_send()
                sum_z(b, c).wait_send()
                gather_z(b, c).wait_send()
                gather_x(b, 0, c).wait_send()
                gather_x(b, 1, c).wait_send()
                relay_first(b, c).wait_send()

            @pl.when(lower)
            def _():
                lift_z(b, c).wait_send()
                half_x(b, c).wait_send()

            @pl.when(upper)
            def _():
                half_x(b, c).wait_send()
                sum_half(b, c).wait_send()

            @pl.when(upper & (sect < last))
            def _():
                relay(b, c).wait_send()

        @pl.when(lower)
        def _():
            mix_z(b, 0).wait_send()
            mix_z(b, 1).wait_send()

        @pl.when(sect == 2)
        def _():
            target_z(b).wait_send()
            target_x(b, 0).wait_send()
            target_x(b, 1).wait_send()

        @pl.when(upper & (sect == last))
        def _():
            def one(t, inner):
                @pl.when((t != s) | swap)
                def _():
                    out_copy(b, t).wait_send()
                return inner

            lax.fori_loop(0, n_seg, one, 0)

        with jax.named_scope("o_wait"):
            wait_for(out.at[b], out_r.at[b])
        return carry

    lax.fori_loop(0, batches, finish, 0)

    @pl.when(lower)
    def _():
        far_copy().wait_send()

    @pl.when(upper)
    def _():
        far_swap().wait_send()
        for k in range(1, tall):
            far_side(k).wait_send()


def on_device(n_seg, n_dp, src, tgt, slen, tlen, win, wout, gain, fgain):
    batches, seq, cols = src.shape
    width = cols * n_seg
    depth, fan = win.shape[1:]
    heads = wout.shape[1]
    rows = seq // GROUP
    any_space = pl.BlockSpec(memory_space=pl.ANY)
    vmem = pl.BlockSpec(memory_space=pltpu.VMEM)
    smem = pl.BlockSpec(memory_space=pltpu.SMEM)
    dma = pltpu.SemaphoreType.DMA
    return pl.pallas_call(
        functools.partial(kernel, n_seg, n_dp),
        out_shape=jax.ShapeDtypeStruct((batches, seq, cols), BF16),
        in_specs=[any_space, any_space, smem, smem, any_space, any_space, vmem, vmem],
        out_specs=any_space,
        scratch_shapes=[
            pltpu.VMEM((depth, fan), BF16),
            pltpu.VMEM((heads, width), BF16),
            pltpu.VMEM((heads, width), BF16),
            pltpu.VMEM((2 * batches, 128), F32),
            pltpu.VMEM((2 * batches, 128), F32),
            pltpu.VMEM((2 * batches, 128), F32),
            pltpu.VMEM((batches, seq, width), BF16),
            pltpu.VMEM((batches, seq, width), BF16),
            pltpu.VMEM((seq, width), BF16),
            pltpu.VMEM((batches, seq, heads), BF16),
            pltpu.VMEM((seq, fan), F32),
            pltpu.VMEM((seq, fan), BF16),
            pltpu.VMEM((batches, seq, heads), BF16),
            pltpu.VMEM((batches, seq, heads), BF16),
            pltpu.VMEM((seq, width), F32),
            pltpu.VMEM((batches, seq, width), BF16),
            pltpu.VMEM((batches, 2 * rows, width), BF16),
            pltpu.VMEM((batches, rows, width), BF16),
            pltpu.VMEM((batches, rows, width), BF16),
            pltpu.VMEM((batches, 2 * rows, width), BF16),
            pltpu.SemaphoreType.REGULAR, dma((2,)), dma, dma, dma((n_dp // 4 + 1,)), dma((n_dp // 4 + 1,)), dma((batches, 2)), dma((batches, 2)),
            dma((batches, GROUP)), dma((batches, GROUP)), dma((batches,)), dma((batches,)),
            dma((batches,)), dma((batches,)), dma((batches, 2)), dma((batches, 2)),
            dma((batches, CHUNKS)), dma((batches, CHUNKS)),
            dma((batches, CHUNKS)), dma((batches, CHUNKS)),
            dma((batches, 2, CHUNKS)), dma((batches, 2, CHUNKS)),
            dma((batches, 2, CHUNKS)), dma((batches, 2, CHUNKS)),
            dma((batches, CHUNKS)), dma((batches, CHUNKS)),
            dma((batches, n_seg)), dma((batches,)),
        ],
        compiler_params=pltpu.CompilerParams(
            collective_id=0, has_side_effects=True, vmem_limit_bytes=56 * 1024 * 1024
        ),
    )(src, tgt, slen, tlen, win, wout, gain, fgain.reshape(1, -1))


def solution(mesh):
    spec = P("dp", None, "segment")
    return jax.shard_map(
        functools.partial(on_device, mesh.shape["segment"], mesh.shape["dp"]),
        mesh=mesh,
        in_specs=(spec, spec, P("dp"), P("dp"), P("segment", None, None), P("segment", None, None), P(), P()),
        out_specs=spec,
        check_vma=False,
    )
```

```python
import functools

import jax
import jax.numpy as jnp
from jax import lax
from jax.experimental import pallas as pl
from jax.experimental.pallas import tpu as pltpu
from jax.sharding import PartitionSpec as P

HEAD = 64
GROUP = 4
CHUNKS = 8
WIDE = 4
PROJ = 4
AHEAD = 1
EARLY = 0
EPS = 1e-06
SCALE = 0.125
MASKED = -1000000000.0
MESH = pl.DeviceIdType.MESH
F32 = jnp.float32
BF16 = jnp.bfloat16


def rms(values, gain):
    return values * lax.rsqrt(jnp.mean(values * values, axis=-1, keepdims=True) + EPS) * gain


def kernel(
    n_seg, n_dp, src, tgt, slen, tlen, win, wout, gain, fgain, out,
    w_in, w_out, w_far, lens_own, lens_far, lens, arr, tg, nb, qs, acc, qkv, mix, mix_far, pf, part, rx, rz, zs, yb,
    go, turn, wsem, lens_s, lens_r, far_s, far_r, mix_s, mix_r, src_s, tgt_s, src_r, tgt_r, tz_s, tz_r, tx_s, tx_r,
    relay_s, relay_r, agz_s, agz_r, agx_s, agx_r, rsx_s, rsx_r, rsz_s, rsz_r, out_s, out_r,
):
    batches, seq, cols = src.shape
    rows = seq // GROUP
    half = seq // 2
    block = cols * n_seg // CHUNKS
    heads = w_out.shape[0]
    s = lax.axis_index("segment")
    sect = s // GROUP
    m = s % GROUP
    zl = m // 2
    xl = m % 2
    x_near = s + 1 - 2 * xl
    d = lax.axis_index("dp")
    flipped = d + 2 - 4 * ((d // 2) % 2)
    alt = d % 2 == 1
    swap = alt & (xl == 1)
    x_dp = jnp.where(alt, flipped, d)
    work_dp = jnp.where(swap, flipped, d)
    core = d % 2
    twin = d + 1 - 2 * core
    own_q = xl * 2 + zl
    z_q = xl * 2 + 1 - zl
    lower = (sect > 0) & (zl == 0)
    upper = (sect > 0) & (zl == 1)
    z_near = s + 2 - 4 * zl
    last = n_seg // GROUP - 1

    load_in = pltpu.make_async_copy(win.at[0], w_in, wsem.at[0])
    load_out = pltpu.make_async_copy(wout.at[0], w_out, wsem.at[1])
    load_in.start()
    load_out.start()

    barrier = pltpu.get_barrier_semaphore()
    for k in range(1, n_seg):
        pl.semaphore_signal(
            barrier, inc=1, device_id={"segment": (s + k) % n_seg}, device_id_type=MESH
        )
    pl.semaphore_signal(
        barrier, inc=1, device_id={"segment": s, "dp": twin}, device_id_type=MESH
    )
    for k in range(1, n_dp // 4):
        pl.semaphore_signal(
            barrier, inc=1, device_id={"segment": s, "dp": (d + 4 * k) % n_dp}, device_id_type=MESH
        )

    @pl.when(alt)
    def _():
        for k in range(n_seg):
            pl.semaphore_signal(
                barrier, inc=1, device_id={"segment": k, "dp": flipped}, device_id_type=MESH
            )

    row = lax.broadcasted_iota(jnp.int32, lens_own.shape, 0)
    table = jnp.zeros(lens_own.shape, F32)
    for k in range(batches):
        table = jnp.where(row == k, slen[k].astype(F32), table)
        table = jnp.where(row == batches + k, tlen[k].astype(F32), table)
    lens_own[...] = table
    with jax.named_scope("barrier"):
        pl.semaphore_wait(barrier, n_seg + n_dp // 4 - 1 + jnp.where(alt, n_seg, 0))

    def remote(src_ref, dst_ref, send, recv, target, target_dp=None):
        return pltpu.make_async_remote_copy(
            src_ref=src_ref, dst_ref=dst_ref, send_sem=send, recv_sem=recv,
            device_id={"segment": target, "dp": d if target_dp is None else target_dp},
            device_id_type=MESH,
        )

    def lens_copy():
        return remote(lens_own, lens_far, lens_s, lens_r, s, flipped)

    @pl.when(swap)
    def _():
        lens_copy().start()

    def wait_for(ref, sem):
        pltpu.make_async_copy(ref, ref, sem).wait()

    def quarter(q):
        return pl.ds(pl.multiple_of(q * rows, rows), rows)

    def strip(c):
        return slice(c * block, (c + 1) * block)

    def wide(c, pieces):
        return slice(c * cols * n_seg // pieces, (c + 1) * cols * n_seg // pieces)

    def strips_of(c, pieces):
        return range(c * CHUNKS // pieces, (c + 1) * CHUNKS // pieces)

    tall = n_dp // 4
    share = heads // (2 * tall)
    y = d // 4

    def far_rows(level):
        return pl.ds(pl.multiple_of((core * tall + level) * share, share), share)

    def far_copy():
        return remote(wout.at[0, far_rows(y)], w_far.at[far_rows(y)], far_s.at[0], far_r.at[0], z_near)

    def far_side(k):
        ref = w_far.at[far_rows(y)]
        return remote(ref, ref, far_s.at[k], far_r.at[k], s, (d + 4 * k) % n_dp)

    def far_swap():
        ref = w_far.at[pl.ds(pl.multiple_of(core * (heads // 2), heads // 2), heads // 2)]
        return remote(ref, ref, far_s.at[tall], far_r.at[tall], s, twin)

    own_cols = pl.ds(pl.multiple_of(s * cols, cols), cols)

    def part_of(t):
        return slice((t % 2 * 2 + t // 2) * rows, (t % 2 * 2 + t // 2 + 1) * rows)

    def spread(given, held, send, recv, first, b, t):
        return remote(
            given.at[b, part_of(t)], held.at[b, part_of(t), own_cols],
            send.at[b, t], recv.at[b], first + t,
            jnp.where(alt, flipped, d) if t % 2 == 1 else d,
        )

    def stays(first, t):
        same = s == first + t
        return same & jnp.logical_not(alt) if t % 2 == 1 else same

    def scatter(given, held, send, recv, first, b):
        for t in range(GROUP):
            @pl.when(jnp.logical_not(stays(first, t)))
            def _():
                spread(given, held, send, recv, first, b, t).start()

            @pl.when(stays(first, t))
            def _():
                pltpu.make_async_copy(
                    given.at[b, part_of(t)], held.at[b, part_of(t), own_cols], recv.at[b]
                ).start()

    def scattered(given, held, send, recv, first, b):
        for t in range(GROUP):
            @pl.when(jnp.logical_not(stays(first, t)))
            def _():
                spread(given, held, send, recv, first, b, t).wait_send()

    def give_source(b, carry):
        scatter(src, arr, src_s, src_r, 0, b)
        return carry

    @pl.when(lower & (sect == 1))
    def _():
        far_copy().start()

    give_source(0, 0)
    give_source(1, 0)

    def give_target(b, carry):
        scatter(tgt, tg, tgt_s, tgt_r, 2 * GROUP, b)
        return carry

    def paced(b, carry):
        give_source(b, carry)
        scattered(src, arr, src_s, src_r, 0, b)
        return carry

    @pl.when(sect == 0)
    def _():
        with jax.named_scope("first_wait"):
            wait_for(arr.at[0, quarter(own_q)], src_r.at[0])

    @pl.when(sect > 0)
    def _():
        scattered(src, arr, src_s, src_r, 0, 0)
        scattered(src, arr, src_s, src_r, 0, 1)
        lax.fori_loop(0, batches, give_target, 0)

    @pl.when(lower & (sect == 2))
    def _():
        far_copy().start()

    def far_share():
        with jax.named_scope("far"):
            far_copy().wait_recv()
            for k in range(1, tall):
                far_side(k).start()

    @pl.when(upper & (sect < last))
    def _():
        far_share()

    @pl.when(sect > 0)
    def _():
        with jax.named_scope("go_wait"):
            pl.semaphore_wait(go, GROUP)

    @pl.when(sect == 1)
    def _():
        lax.fori_loop(2, batches, give_source, 0)

    @pl.when(sect > 1)
    def _():
        with jax.named_scope("paced"):
            lax.fori_loop(2, batches, paced, 0)

    @pl.when(lower & (sect > 2))
    def _():
        far_copy().start()

    def go_ahead():
        for k in range(GROUP, n_seg):
            pl.semaphore_signal(
                go, inc=1, device_id={"segment": k, "dp": work_dp}, device_id_type=MESH
            )
        lax.fori_loop(2, batches, give_source, 0)

    def side_rows(side):
        return pl.ds(pl.multiple_of(side * half, half), half)

    def relay_first(b, c):
        return remote(
            yb.at[b, :rows, strip(c)], arr.at[b, quarter(own_q), strip(c)], relay_s.at[b, c],
            relay_r.at[b, c], GROUP + xl,
        )

    def relay(b, c):
        return remote(
            yb.at[b, :, strip(c)], arr.at[b, side_rows(xl), strip(c)],
            relay_s.at[b, c], relay_r.at[b, c], (s + 2) % n_seg,
        )

    def gather_z(b, c):
        ref = arr.at[b, quarter(own_q), strip(c)]
        return remote(ref, ref, agz_s.at[b, c], agz_r.at[b, c], z_near)

    def gather_x(b, which, c):
        ref = arr.at[b, quarter(own_q if which == 0 else z_q), strip(c)]
        return remote(ref, ref, agx_s.at[b, which, c], agx_r.at[b, which, c], x_near, x_dp)

    def lift_z(b, c):
        ref = arr.at[b, side_rows(xl), strip(c)]
        return remote(ref, ref, agz_s.at[b, c], agz_r.at[b, c], z_near)

    def half_x(b, c):
        ref = arr.at[b, side_rows(xl), strip(c)]
        return remote(ref, ref, agx_s.at[b, 0, c], agx_r.at[b, 0, c], x_near, x_dp)

    def mix_z(b, k):
        side = slice(k * heads // 2, (k + 1) * heads // 2)
        return remote(
            mix.at[b, :, side], mix_far.at[b, :, side], mix_s.at[b, k], mix_r.at[b, k], z_near
        )

    def target_z(b):
        ref = tg.at[b, quarter(own_q)]
        return remote(ref, ref, tz_s.at[b], tz_r.at[b], z_near)

    def target_x(b, which):
        ref = tg.at[b, quarter(own_q if which == 0 else z_q)]
        return remote(ref, ref, tx_s.at[b, which], tx_r.at[b, which], x_near, x_dp)

    def sum_x(b, which, c):
        wanted = (1 - xl) * 2 + (1 - zl if which == 0 else zl)
        return remote(
            part.at[b, quarter(wanted), strip(c)], rx.at[b, which * rows:(which + 1) * rows, strip(c)],
            rsx_s.at[b, which, c], rsx_r.at[b, which, c], x_near, x_dp,
        )

    def sum_half(b, c):
        return remote(
            part.at[b, side_rows(1 - xl), strip(c)], rx.at[b, :, strip(c)],
            rsx_s.at[b, 0, c], rsx_r.at[b, 0, c], x_near, x_dp,
        )

    def sum_z(b, c):
        return remote(zs.at[b, :, strip(c)], rz.at[b, :, strip(c)], rsz_s.at[b, c], rsz_r.at[b, c], z_near)

    def out_copy(b, t):
        return remote(
            yb.at[b, :, pl.ds(t * cols if isinstance(t, int) else pl.multiple_of(t * cols, cols), cols)],
            out.at[b, pl.ds(pl.multiple_of(xl * half, half), half)], out_s.at[b, t], out_r.at[b], t, work_dp,
        )

    def step_r(b, waits=True):
        if waits:
            with jax.named_scope("r_wait"):
                wait_for(arr.at[b, quarter(own_q)], src_r.at[b])
        for c in range(CHUNKS):
            gather_z(b, c).start()
            gather_x(b, 0, c).start()

    def step_f(b, c):
        with jax.named_scope("f_wait"):
            gather_z(b, c).wait_recv()
        gather_x(b, 1, c).start()

    def step_r2(b, c):
        with jax.named_scope("r_wait"):
            wait_for(arr.at[b, side_rows(xl), strip(c)], relay_r.at[b, c])
        lift_z(b, c).start()
        half_x(b, c).start()

    def step_f2(b, c):
        with jax.named_scope("f_wait"):
            lift_z(b, c).wait_recv()
        half_x(b, c).start()

    own_gain = gain[pl.ds(sect, 1), :]

    strip_gain = jnp.where(sect == 2, fgain[...], own_gain)

    def project(b, wait):
        squares = jnp.zeros((seq, 1), F32)
        for w in range(PROJ):
            for c in strips_of(w, PROJ):
                wait(c)
            span = wide(w, PROJ)
            held = arr[b, :, span].astype(F32)
            squares = squares + jnp.sum(held * held, axis=-1, keepdims=True)
            nb[:, span] = (held * strip_gain[:, span]).astype(BF16)
            with jax.named_scope("kv_dot"):
                grown = jnp.dot(nb[:, span], w_in[span, :], preferred_element_type=F32)
                if w == 0:
                    acc[...] = grown
                elif w < PROJ - 1:
                    acc[...] += grown
                else:
                    scale = lax.rsqrt(squares / (cols * n_seg) + EPS)
                    qkv[...] = ((acc[...] + grown) * scale).astype(BF16)

        @pl.when(sect == 2)
        def _():
            qkv[:, :heads] = qs[b]

    def attend(b):
        length = lens[pl.ds(jnp.where(sect == last, batches, 0) + b, 1), :seq]
        query_pos = lax.broadcasted_iota(jnp.int32, (seq, seq), 0)
        key_pos = lax.broadcasted_iota(jnp.int32, (seq, seq), 1)
        limit = jnp.where(sect == last, query_pos, seq)
        allowed = (key_pos.astype(F32) < length) & (key_pos <= limit)
        allowed = jnp.concatenate([allowed, allowed], axis=0)
        pair = 2 * HEAD
        low = lax.broadcasted_iota(jnp.int32, (seq, pair), 1) < HEAD
        for j in range(heads // pair):
            q2 = qkv[:, j * pair:(j + 1) * pair]
            k2 = qkv[:, heads + j * pair:heads + (j + 1) * pair]
            v2 = qkv[:, 2 * heads + j * pair:2 * heads + (j + 1) * pair]
            zero = jnp.zeros_like(q2)
            stacked = jnp.concatenate([jnp.where(low, q2, zero), jnp.where(low, zero, q2)], axis=0)
            scores = lax.dot_general(
                stacked, k2, (((1,), (1,)), ((), ())), preferred_element_type=F32
            ) * SCALE
            scores = jnp.where(allowed, scores, MASKED)
            grown = jnp.exp(scores - jnp.max(scores, axis=-1, keepdims=True))
            weights = (grown / jnp.sum(grown, axis=-1, keepdims=True)).astype(BF16)
            both = jnp.dot(weights, v2, preferred_element_type=F32)
            mix[b, :, j * pair:(j + 1) * pair] = jnp.where(low, both[:seq], both[seq:]).astype(BF16)
            if (j + 1) * pair * 2 == heads:
                @pl.when(lower)
                def _():
                    mix_z(b, 0).start()

    def step_z(b, c):
        with jax.named_scope("z_wait"):
            sum_x(b, 0, c).wait_recv()
        zs[b, :, strip(c)] = (pf[quarter(z_q), strip(c)] + rx[b, :rows, strip(c)].astype(F32)).astype(BF16)
        sum_z(b, c).start()

    def step_y(b, c):
        with jax.named_scope("y_wait"):
            sum_x(b, 1, c).wait_recv()
            sum_z(b, c).wait_recv()
        total = (
            pf[quarter(own_q), strip(c)] + rx[b, rows:, strip(c)].astype(F32)
            + rz[b, :, strip(c)].astype(F32)
        )
        yb[b, :rows, strip(c)] = (arr[b, quarter(own_q), strip(c)].astype(F32) + total).astype(BF16)
        relay_first(b, c).start()

    def step_y2(b, c):
        with jax.named_scope("y_wait"):
            sum_half(b, c).wait_recv()
        mine = side_rows(xl)
        total = pf[mine, strip(c)] + rx[b, :, strip(c)].astype(F32)

        @pl.when(sect == 2)
        def _():
            yb[b, :, strip(c)] = (tg[b, mine, strip(c)].astype(F32) + total).astype(BF16)

        @pl.when(sect != 2)
        def _():
            yb[b, :, strip(c)] = (arr[b, mine, strip(c)].astype(F32) + total).astype(BF16)

        @pl.when(sect < last)
        def _():
            relay(b, c).start()

        @pl.when(sect == last)
        def _():
            for t in range(c * n_seg // CHUNKS, (c + 1) * n_seg // CHUNKS):
                @pl.when((t != s) | swap)
                def _():
                    out_copy(b, t).start()

                @pl.when((t == s) & jnp.logical_not(swap))
                def _():
                    pltpu.make_async_copy(
                        yb.at[b, :, own_cols],
                        out.at[b, pl.ds(pl.multiple_of(xl * half, half), half)], out_r.at[b],
                    ).start()

    @pl.when(swap)
    def _():
        lens_copy().wait()
        lens[...] = lens_far[...]

    @pl.when(jnp.logical_not(swap))
    def _():
        lens[...] = lens_own[...]

    with jax.named_scope("load"):
        load_in.wait()
        load_out.wait()

    @pl.when(sect == 2)
    def _():
        def first(b, carry):
            wait_for(tg.at[b, quarter(own_q)], tgt_r.at[b])
            target_z(b).start()
            target_x(b, 0).start()
            return carry

        lax.fori_loop(0, batches, first, 0)

    @pl.when(upper & (sect == last))
    def _():
        far_share()

    @pl.when(sect == 2)
    def _():
        def second(b, carry):
            target_z(b).wait_recv()
            target_x(b, 1).start()
            return carry

        lax.fori_loop(0, batches, second, 0)

        def third(b, carry):
            target_x(b, 0).wait_recv()
            target_x(b, 1).wait_recv()
            nb[...] = rms(tg[b].astype(F32), own_gain).astype(BF16)
            qs[b] = jnp.dot(nb[...], w_in[:, :heads], preferred_element_type=F32).astype(BF16)
            return carry

        with jax.named_scope("target_q"):
            lax.fori_loop(0, batches, third, 0)

    @pl.when(upper)
    def _():
        with jax.named_scope("far_side"):
            for k in range(1, tall):
                wait_for(w_far.at[far_rows((y + tall - k) % tall)], far_r.at[k])
            far_swap().start()

    @pl.when(sect == 0)
    def _():
        step_r(0, False)
        lax.fori_loop(0, batches, give_target, 0)
        for c in range(CHUNKS):
            step_f(0, c)
        step_r(1)

    @pl.when(upper)
    def _():
        for c in range(CHUNKS):
            step_f2(0, c)
        far_swap().wait_recv()

    def main(b, carry):
        more = b < batches - 1

        @pl.when(lower)
        def _():
            for c in range(CHUNKS):
                step_r2(b, c)

        @pl.when(more & (sect == 0) & (b > 0))
        def _():
            step_r(b + 1)

        def arrived(c):
            with jax.named_scope("c_wait"):
                @pl.when(sect == 0)
                def _():
                    gather_x(b, 0, c).wait_recv()
                    gather_x(b, 1, c).wait_recv()

                @pl.when(sect > 0)
                def _():
                    half_x(b, c).wait_recv()

        @pl.when((sect == 0) & (b > 0) & (core == 0))
        def _():
            pl.semaphore_signal(
                turn, inc=1, device_id={"segment": s, "dp": twin}, device_id_type=MESH
            )

        @pl.when((sect == 0) & (b > 0) & (core == 1))
        def _():
            pl.semaphore_wait(turn, 1)

        project(b, arrived)

        @pl.when((sect == 0) & (b == 0))
        def _():
            go_ahead()
        attend(b)

        @pl.when(lower)
        def _():
            mix_z(b, 1).start()

        @pl.when(sect == 0)
        def _():
            for w in range(WIDE):
                with jax.named_scope("out_dot"):
                    total = jnp.dot(mix[b], w_out[:, wide(w, WIDE)], preferred_element_type=F32)
                    pf[:, wide(w, WIDE)] = total
                    part[b, :, wide(w, WIDE)] = total.astype(BF16)
                for c in strips_of(w, WIDE):
                    sum_x(b, 0, c).start()
            for c in range(CHUNKS):
                sum_x(b, 1, c).start()


            @pl.when(more)
            def _():
                for c in range(CHUNKS):
                    step_f(b + 1, c)

            for c in range(CHUNKS):
                step_z(b, c)
            for c in range(CHUNKS):
                step_y(b, c)

        @pl.when(upper)
        def _():
            @pl.when(more)
            def _():
                for c in range(EARLY):
                    step_f2(b + 1, c)

            with jax.named_scope("mix_wait"):
                mix_z(b, 0).wait_recv()
                mix_z(b, 1).wait_recv()
            for w in range(WIDE):
                with jax.named_scope("out_dot2"):
                    total = jnp.dot(mix[b], w_out[:, wide(w, WIDE)], preferred_element_type=F32)
                    total = total + jnp.dot(mix_far[b], w_far[:, wide(w, WIDE)], preferred_element_type=F32)
                    pf[:, wide(w, WIDE)] = total
                    part[b, :, wide(w, WIDE)] = total.astype(BF16)
                for c in strips_of(w, WIDE):
                    sum_half(b, c).start()

            @pl.when(b == 0)
            def _():
                for c in range(CHUNKS):
                    step_y2(b, c)
                    if c > 0:
                        step_f2(b + 1, c - 1)
                step_f2(b + 1, CHUNKS - 1)

            @pl.when(b > 0)
            def _():
                for c in range(CHUNKS):
                    @pl.when(more)
                    def _():
                        step_f2(b + 1, c)

                    step_y2(b, c)
        return carry

    lax.fori_loop(0, batches, main, 0)

    def finish(b, carry):
        @pl.when((sect == 0) | ((sect == 1) & (b > 1)))
        def _():
            scattered(src, arr, src_s, src_r, 0, b)

        scattered(tgt, tg, tgt_s, tgt_r, 2 * GROUP, b)
        for c in range(CHUNKS):
            @pl.when(sect == 0)
            def _():
                sum_x(b, 0, c).wait_send()
                sum_x(b, 1, c).wait_send()
                sum_z(b, c).wait_send()
                gather_z(b, c).wait_send()
                gather_x(b, 0, c).wait_send()
                gather_x(b, 1, c).wait_send()
                relay_first(b, c).wait_send()

            @pl.when(lower)
            def _():
                lift_z(b, c).wait_send()
                half_x(b, c).wait_send()

            @pl.when(upper)
            def _():
                half_x(b, c).wait_send()
                sum_half(b, c).wait_send()

            @pl.when(upper & (sect < last))
            def _():
                relay(b, c).wait_send()

        @pl.when(lower)
        def _():
            mix_z(b, 0).wait_send()
            mix_z(b, 1).wait_send()

        @pl.when(sect == 2)
        def _():
            target_z(b).wait_send()
            target_x(b, 0).wait_send()
            target_x(b, 1).wait_send()

        @pl.when(upper & (sect == last))
        def _():
            def one(t, inner):
                @pl.when((t != s) | swap)
                def _():
                    out_copy(b, t).wait_send()
                return inner

            lax.fori_loop(0, n_seg, one, 0)

        with jax.named_scope("o_wait"):
            wait_for(out.at[b], out_r.at[b])
        return carry

    lax.fori_loop(0, batches, finish, 0)

    @pl.when(lower)
    def _():
        far_copy().wait_send()

    @pl.when(upper)
    def _():
        far_swap().wait_send()
        for k in range(1, tall):
            far_side(k).wait_send()


def on_device(n_seg, n_dp, src, tgt, slen, tlen, win, wout, gain, fgain):
    batches, seq, cols = src.shape
    width = cols * n_seg
    depth, fan = win.shape[1:]
    heads = wout.shape[1]
    rows = seq // GROUP
    any_space = pl.BlockSpec(memory_space=pl.ANY)
    vmem = pl.BlockSpec(memory_space=pltpu.VMEM)
    smem = pl.BlockSpec(memory_space=pltpu.SMEM)
    dma = pltpu.SemaphoreType.DMA
    return pl.pallas_call(
        functools.partial(kernel, n_seg, n_dp),
        out_shape=jax.ShapeDtypeStruct((batches, seq, cols), BF16),
        in_specs=[any_space, any_space, smem, smem, any_space, any_space, vmem, vmem],
        out_specs=any_space,
        scratch_shapes=[
            pltpu.VMEM((depth, fan), BF16),
            pltpu.VMEM((heads, width), BF16),
            pltpu.VMEM((heads, width), BF16),
            pltpu.VMEM((2 * batches, 128), F32),
            pltpu.VMEM((2 * batches, 128), F32),
            pltpu.VMEM((2 * batches, 128), F32),
            pltpu.VMEM((batches, seq, width), BF16),
            pltpu.VMEM((batches, seq, width), BF16),
            pltpu.VMEM((seq, width), BF16),
            pltpu.VMEM((batches, seq, heads), BF16),
            pltpu.VMEM((seq, fan), F32),
            pltpu.VMEM((seq, fan), BF16),
            pltpu.VMEM((batches, seq, heads), BF16),
            pltpu.VMEM((batches, seq, heads), BF16),
            pltpu.VMEM((seq, width), F32),
            pltpu.VMEM((batches, seq, width), BF16),
            pltpu.VMEM((batches, 2 * rows, width), BF16),
            pltpu.VMEM((batches, rows, width), BF16),
            pltpu.VMEM((batches, rows, width), BF16),
            pltpu.VMEM((batches, 2 * rows, width), BF16),
            pltpu.SemaphoreType.REGULAR, pltpu.SemaphoreType.REGULAR, dma((2,)), dma, dma, dma((n_dp // 4 + 1,)), dma((n_dp // 4 + 1,)), dma((batches, 2)), dma((batches, 2)),
            dma((batches, GROUP)), dma((batches, GROUP)), dma((batches,)), dma((batches,)),
            dma((batches,)), dma((batches,)), dma((batches, 2)), dma((batches, 2)),
            dma((batches, CHUNKS)), dma((batches, CHUNKS)),
            dma((batches, CHUNKS)), dma((batches, CHUNKS)),
            dma((batches, 2, CHUNKS)), dma((batches, 2, CHUNKS)),
            dma((batches, 2, CHUNKS)), dma((batches, 2, CHUNKS)),
            dma((batches, CHUNKS)), dma((batches, CHUNKS)),
            dma((batches, n_seg)), dma((batches,)),
        ],
        compiler_params=pltpu.CompilerParams(
            collective_id=0, has_side_effects=True, vmem_limit_bytes=56 * 1024 * 1024
        ),
    )(src, tgt, slen, tlen, win, wout, gain, fgain.reshape(1, -1))


def solution(mesh):
    spec = P("dp", None, "segment")
    return jax.shard_map(
        functools.partial(on_device, mesh.shape["segment"], mesh.shape["dp"]),
        mesh=mesh,
        in_specs=(spec, spec, P("dp"), P("dp"), P("segment", None, None), P("segment", None, None), P(), P()),
        out_specs=spec,
        check_vma=False,
    )
```

```python
import functools

import jax
import jax.numpy as jnp
from jax import lax
from jax.experimental import pallas as pl
from jax.experimental.pallas import tpu as pltpu
from jax.sharding import PartitionSpec as P

HEAD = 64
GROUP = 4
CHUNKS = 8
WIDE = 4
PROJ = 4
AHEAD = 1
EARLY = 0
EPS = 1e-06
SCALE = 0.125
MASKED = -1000000000.0
MESH = pl.DeviceIdType.MESH
F32 = jnp.float32
BF16 = jnp.bfloat16


def rms(values, gain):
    return values * lax.rsqrt(jnp.mean(values * values, axis=-1, keepdims=True) + EPS) * gain


def kernel(
    n_seg, n_dp, src, tgt, slen, tlen, win, wout, gain, fgain, out,
    w_in, w_out, w_far, lens_own, lens_far, lens, arr, tg, nb, qs, acc, qkv, mix, mix_far, pf, part, rx, rz, zs, yb,
    go, turn, wsem, lens_s, lens_r, far_s, far_r, mix_s, mix_r, src_s, tgt_s, src_r, tgt_r, tz_s, tz_r, tx_s, tx_r,
    relay_s, relay_r, agz_s, agz_r, agx_s, agx_r, rsx_s, rsx_r, rsz_s, rsz_r, out_s, out_r,
):
    batches, seq, cols = src.shape
    rows = seq // GROUP
    half = seq // 2
    block = cols * n_seg // CHUNKS
    heads = w_out.shape[0]
    s = lax.axis_index("segment")
    sect = s // GROUP
    m = s % GROUP
    zl = m // 2
    xl = m % 2
    x_near = s + 1 - 2 * xl
    d = lax.axis_index("dp")
    flipped = d + 2 - 4 * ((d // 2) % 2)
    alt = d % 2 == 1
    swap = alt & (xl == 1)
    x_dp = jnp.where(alt, flipped, d)
    work_dp = jnp.where(swap, flipped, d)
    core = d % 2
    twin = d + 1 - 2 * core
    own_q = xl * 2 + zl
    z_q = xl * 2 + 1 - zl
    lower = (sect > 0) & (zl == 0)
    upper = (sect > 0) & (zl == 1)
    z_near = s + 2 - 4 * zl
    last = n_seg // GROUP - 1

    load_in = pltpu.make_async_copy(win.at[0], w_in, wsem.at[0])
    load_out = pltpu.make_async_copy(wout.at[0], w_out, wsem.at[1])
    load_in.start()
    load_out.start()

    barrier = pltpu.get_barrier_semaphore()
    for k in range(1, n_seg):
        pl.semaphore_signal(
            barrier, inc=1, device_id={"segment": (s + k) % n_seg}, device_id_type=MESH
        )
    pl.semaphore_signal(
        barrier, inc=1, device_id={"segment": s, "dp": twin}, device_id_type=MESH
    )
    for k in range(1, n_dp // 4):
        pl.semaphore_signal(
            barrier, inc=1, device_id={"segment": s, "dp": (d + 4 * k) % n_dp}, device_id_type=MESH
        )

    @pl.when(alt)
    def _():
        for k in range(n_seg):
            pl.semaphore_signal(
                barrier, inc=1, device_id={"segment": k, "dp": flipped}, device_id_type=MESH
            )

    row = lax.broadcasted_iota(jnp.int32, lens_own.shape, 0)
    table = jnp.zeros(lens_own.shape, F32)
    for k in range(batches):
        table = jnp.where(row == k, slen[k].astype(F32), table)
        table = jnp.where(row == batches + k, tlen[k].astype(F32), table)
    lens_own[...] = table
    with jax.named_scope("barrier"):
        pl.semaphore_wait(barrier, n_seg + n_dp // 4 - 1 + jnp.where(alt, n_seg, 0))

    def remote(src_ref, dst_ref, send, recv, target, target_dp=None):
        return pltpu.make_async_remote_copy(
            src_ref=src_ref, dst_ref=dst_ref, send_sem=send, recv_sem=recv,
            device_id={"segment": target, "dp": d if target_dp is None else target_dp},
            device_id_type=MESH,
        )

    def lens_copy():
        return remote(lens_own, lens_far, lens_s, lens_r, s, flipped)

    @pl.when(swap)
    def _():
        lens_copy().start()

    def wait_for(ref, sem):
        pltpu.make_async_copy(ref, ref, sem).wait()

    def quarter(q):
        return pl.ds(pl.multiple_of(q * rows, rows), rows)

    def strip(c):
        return slice(c * block, (c + 1) * block)

    def wide(c, pieces):
        return slice(c * cols * n_seg // pieces, (c + 1) * cols * n_seg // pieces)

    def strips_of(c, pieces):
        return range(c * CHUNKS // pieces, (c + 1) * CHUNKS // pieces)

    tall = n_dp // 4
    share = heads // (2 * tall)
    y = d // 4

    def far_rows(level):
        return pl.ds(pl.multiple_of((core * tall + level) * share, share), share)

    def far_copy():
        return remote(wout.at[0, far_rows(y)], w_far.at[far_rows(y)], far_s.at[0], far_r.at[0], z_near)

    def far_side(k):
        ref = w_far.at[far_rows(y)]
        return remote(ref, ref, far_s.at[k], far_r.at[k], s, (d + 4 * k) % n_dp)

    def far_swap():
        ref = w_far.at[pl.ds(pl.multiple_of(core * (heads // 2), heads // 2), heads // 2)]
        return remote(ref, ref, far_s.at[tall], far_r.at[tall], s, twin)

    own_cols = pl.ds(pl.multiple_of(s * cols, cols), cols)

    def part_of(t):
        return slice((t % 2 * 2 + t // 2) * rows, (t % 2 * 2 + t // 2 + 1) * rows)

    def spread(given, held, send, recv, first, b, t):
        return remote(
            given.at[b, part_of(t)], held.at[b, part_of(t), own_cols],
            send.at[b, t], recv.at[b], first + t,
            jnp.where(alt, flipped, d) if t % 2 == 1 else d,
        )

    def stays(first, t):
        same = s == first + t
        return same & jnp.logical_not(alt) if t % 2 == 1 else same

    def scatter(given, held, send, recv, first, b):
        for t in range(GROUP):
            @pl.when(jnp.logical_not(stays(first, t)))
            def _():
                spread(given, held, send, recv, first, b, t).start()

            @pl.when(stays(first, t))
            def _():
                pltpu.make_async_copy(
                    given.at[b, part_of(t)], held.at[b, part_of(t), own_cols], recv.at[b]
                ).start()

    def scattered(given, held, send, recv, first, b):
        for t in range(GROUP):
            @pl.when(jnp.logical_not(stays(first, t)))
            def _():
                spread(given, held, send, recv, first, b, t).wait_send()

    def give_source(b, carry):
        scatter(src, arr, src_s, src_r, 0, b)
        return carry

    @pl.when(lower & (sect == 1))
    def _():
        far_copy().start()

    give_source(0, 0)
    give_source(1, 0)

    def give_target(b, carry):
        scatter(tgt, tg, tgt_s, tgt_r, 2 * GROUP, b)
        return carry

    def paced(b, carry):
        give_source(b, carry)
        scattered(src, arr, src_s, src_r, 0, b)
        return carry

    @pl.when(sect == 0)
    def _():
        with jax.named_scope("first_wait"):
            wait_for(arr.at[0, quarter(own_q)], src_r.at[0])

    @pl.when(sect > 0)
    def _():
        scattered(src, arr, src_s, src_r, 0, 0)
        scattered(src, arr, src_s, src_r, 0, 1)
        lax.fori_loop(0, batches, give_target, 0)

    @pl.when(lower & (sect == 2))
    def _():
        far_copy().start()

    def far_share():
        with jax.named_scope("far"):
            far_copy().wait_recv()
            for k in range(1, tall):
                far_side(k).start()

    @pl.when(upper & (sect < last))
    def _():
        far_share()

    @pl.when(sect > 0)
    def _():
        with jax.named_scope("go_wait"):
            pl.semaphore_wait(go, GROUP)

    @pl.when(sect == 1)
    def _():
        lax.fori_loop(2, batches, give_source, 0)

    @pl.when(sect > 1)
    def _():
        with jax.named_scope("paced"):
            lax.fori_loop(2, batches, paced, 0)

    @pl.when(lower & (sect > 2))
    def _():
        far_copy().start()

    def go_ahead():
        for k in range(GROUP, n_seg):
            pl.semaphore_signal(
                go, inc=1, device_id={"segment": k, "dp": work_dp}, device_id_type=MESH
            )
        lax.fori_loop(2, batches, give_source, 0)

    def side_rows(side):
        return pl.ds(pl.multiple_of(side * half, half), half)

    def relay_first(b, c):
        return remote(
            yb.at[b, :rows, strip(c)], arr.at[b, quarter(own_q), strip(c)], relay_s.at[b, c],
            relay_r.at[b, c], GROUP + xl,
        )

    def relay(b, c):
        return remote(
            yb.at[b, :, strip(c)], arr.at[b, side_rows(xl), strip(c)],
            relay_s.at[b, c], relay_r.at[b, c], (s + 2) % n_seg,
        )

    def gather_z(b, c):
        ref = arr.at[b, quarter(own_q), strip(c)]
        return remote(ref, ref, agz_s.at[b, c], agz_r.at[b, c], z_near)

    def gather_x(b, which, c):
        ref = arr.at[b, quarter(own_q if which == 0 else z_q), strip(c)]
        return remote(ref, ref, agx_s.at[b, which, c], agx_r.at[b, which, c], x_near, x_dp)

    def lift_z(b, c):
        ref = arr.at[b, side_rows(xl), strip(c)]
        return remote(ref, ref, agz_s.at[b, c], agz_r.at[b, c], z_near)

    def half_x(b, c):
        ref = arr.at[b, side_rows(xl), strip(c)]
        return remote(ref, ref, agx_s.at[b, 0, c], agx_r.at[b, 0, c], x_near, x_dp)

    def mix_z(b, k):
        side = slice(k * heads // 2, (k + 1) * heads // 2)
        return remote(
            mix.at[b, :, side], mix_far.at[b, :, side], mix_s.at[b, k], mix_r.at[b, k], z_near
        )

    def target_z(b):
        ref = tg.at[b, quarter(own_q)]
        return remote(ref, ref, tz_s.at[b], tz_r.at[b], z_near)

    def target_x(b, which):
        ref = tg.at[b, quarter(own_q if which == 0 else z_q)]
        return remote(ref, ref, tx_s.at[b, which], tx_r.at[b, which], x_near, x_dp)

    def sum_x(b, which, c):
        wanted = (1 - xl) * 2 + (1 - zl if which == 0 else zl)
        return remote(
            part.at[b, quarter(wanted), strip(c)], rx.at[b, which * rows:(which + 1) * rows, strip(c)],
            rsx_s.at[b, which, c], rsx_r.at[b, which, c], x_near, x_dp,
        )

    def sum_half(b, c):
        return remote(
            part.at[b, side_rows(1 - xl), strip(c)], rx.at[b, :, strip(c)],
            rsx_s.at[b, 0, c], rsx_r.at[b, 0, c], x_near, x_dp,
        )

    def sum_z(b, c):
        return remote(zs.at[b, :, strip(c)], rz.at[b, :, strip(c)], rsz_s.at[b, c], rsz_r.at[b, c], z_near)

    def out_copy(b, t):
        return remote(
            yb.at[b, :, pl.ds(t * cols if isinstance(t, int) else pl.multiple_of(t * cols, cols), cols)],
            out.at[b, pl.ds(pl.multiple_of(xl * half, half), half)], out_s.at[b, t], out_r.at[b], t, work_dp,
        )

    def step_r(b, waits=True):
        if waits:
            with jax.named_scope("r_wait"):
                wait_for(arr.at[b, quarter(own_q)], src_r.at[b])
        for c in range(CHUNKS):
            gather_z(b, c).start()
            gather_x(b, 0, c).start()

    def step_f(b, c):
        with jax.named_scope("f_wait"):
            gather_z(b, c).wait_recv()
        gather_x(b, 1, c).start()

    def step_r2(b, c):
        with jax.named_scope("r_wait"):
            wait_for(arr.at[b, side_rows(xl), strip(c)], relay_r.at[b, c])
        lift_z(b, c).start()
        half_x(b, c).start()

    def step_f2(b, c):
        with jax.named_scope("f_wait"):
            lift_z(b, c).wait_recv()
        half_x(b, c).start()

    own_gain = gain[pl.ds(sect, 1), :]

    strip_gain = jnp.where(sect == 2, fgain[...], own_gain)

    def project(b, wait):
        squares = jnp.zeros((seq, 1), F32)
        for w in range(PROJ):
            for c in strips_of(w, PROJ):
                wait(c)
            span = wide(w, PROJ)
            held = arr[b, :, span].astype(F32)
            squares = squares + jnp.sum(held * held, axis=-1, keepdims=True)
            nb[:, span] = (held * strip_gain[:, span]).astype(BF16)
            with jax.named_scope("kv_dot"):
                grown = jnp.dot(nb[:, span], w_in[span, :], preferred_element_type=F32)
                if w == 0:
                    acc[...] = grown
                elif w < PROJ - 1:
                    acc[...] += grown
                else:
                    scale = lax.rsqrt(squares / (cols * n_seg) + EPS)
                    qkv[...] = ((acc[...] + grown) * scale).astype(BF16)

        @pl.when(sect == 2)
        def _():
            qkv[:, :heads] = qs[b]

    def attend(b):
        length = lens[pl.ds(jnp.where(sect == last, batches, 0) + b, 1), :seq]
        query_pos = lax.broadcasted_iota(jnp.int32, (seq, seq), 0)
        key_pos = lax.broadcasted_iota(jnp.int32, (seq, seq), 1)
        limit = jnp.where(sect == last, query_pos, seq)
        allowed = (key_pos.astype(F32) < length) & (key_pos <= limit)
        allowed = jnp.concatenate([allowed, allowed], axis=0)
        pair = 2 * HEAD
        low = lax.broadcasted_iota(jnp.int32, (seq, pair), 1) < HEAD
        for j in range(heads // pair):
            q2 = qkv[:, j * pair:(j + 1) * pair]
            k2 = qkv[:, heads + j * pair:heads + (j + 1) * pair]
            v2 = qkv[:, 2 * heads + j * pair:2 * heads + (j + 1) * pair]
            zero = jnp.zeros_like(q2)
            stacked = jnp.concatenate([jnp.where(low, q2, zero), jnp.where(low, zero, q2)], axis=0)
            scores = lax.dot_general(
                stacked, k2, (((1,), (1,)), ((), ())), preferred_element_type=F32
            ) * SCALE
            scores = jnp.where(allowed, scores, MASKED)
            grown = jnp.exp(scores - jnp.max(scores, axis=-1, keepdims=True))
            weights = (grown / jnp.sum(grown, axis=-1, keepdims=True)).astype(BF16)
            both = jnp.dot(weights, v2, preferred_element_type=F32)
            mix[b, :, j * pair:(j + 1) * pair] = jnp.where(low, both[:seq], both[seq:]).astype(BF16)
            if (j + 1) * pair * 2 == heads:
                @pl.when(lower)
                def _():
                    mix_z(b, 0).start()

    def step_z(b, c):
        with jax.named_scope("z_wait"):
            sum_x(b, 0, c).wait_recv()
        zs[b, :, strip(c)] = (pf[quarter(z_q), strip(c)] + rx[b, :rows, strip(c)].astype(F32)).astype(BF16)
        sum_z(b, c).start()

    def step_y(b, c):
        with jax.named_scope("y_wait"):
            sum_x(b, 1, c).wait_recv()
            sum_z(b, c).wait_recv()
        total = (
            pf[quarter(own_q), strip(c)] + rx[b, rows:, strip(c)].astype(F32)
            + rz[b, :, strip(c)].astype(F32)
        )
        yb[b, :rows, strip(c)] = (arr[b, quarter(own_q), strip(c)].astype(F32) + total).astype(BF16)
        relay_first(b, c).start()

    def step_y2(b, c):
        with jax.named_scope("y_wait"):
            sum_half(b, c).wait_recv()
        mine = side_rows(xl)
        total = pf[mine, strip(c)] + rx[b, :, strip(c)].astype(F32)

        @pl.when(sect == 2)
        def _():
            yb[b, :, strip(c)] = (tg[b, mine, strip(c)].astype(F32) + total).astype(BF16)

        @pl.when(sect != 2)
        def _():
            yb[b, :, strip(c)] = (arr[b, mine, strip(c)].astype(F32) + total).astype(BF16)

        @pl.when(sect < last)
        def _():
            relay(b, c).start()

        @pl.when(sect == last)
        def _():
            for t in range(c * n_seg // CHUNKS, (c + 1) * n_seg // CHUNKS):
                @pl.when((t != s) | swap)
                def _():
                    out_copy(b, t).start()

                @pl.when((t == s) & jnp.logical_not(swap))
                def _():
                    pltpu.make_async_copy(
                        yb.at[b, :, own_cols],
                        out.at[b, pl.ds(pl.multiple_of(xl * half, half), half)], out_r.at[b],
                    ).start()

    @pl.when(swap)
    def _():
        lens_copy().wait()
        lens[...] = lens_far[...]

    @pl.when(jnp.logical_not(swap))
    def _():
        lens[...] = lens_own[...]

    with jax.named_scope("load"):
        load_in.wait()
        load_out.wait()

    @pl.when(sect == 2)
    def _():
        def first(b, carry):
            wait_for(tg.at[b, quarter(own_q)], tgt_r.at[b])
            target_z(b).start()
            target_x(b, 0).start()
            return carry

        lax.fori_loop(0, batches, first, 0)

    @pl.when(upper & (sect == last))
    def _():
        far_share()

    @pl.when(sect == 2)
    def _():
        def second(b, carry):
            target_z(b).wait_recv()
            target_x(b, 1).start()
            return carry

        lax.fori_loop(0, batches, second, 0)

        def third(b, carry):
            target_x(b, 0).wait_recv()
            target_x(b, 1).wait_recv()
            nb[...] = rms(tg[b].astype(F32), own_gain).astype(BF16)
            qs[b] = jnp.dot(nb[...], w_in[:, :heads], preferred_element_type=F32).astype(BF16)
            return carry

        with jax.named_scope("target_q"):
            lax.fori_loop(0, batches, third, 0)

    @pl.when(upper)
    def _():
        with jax.named_scope("far_side"):
            for k in range(1, tall):
                wait_for(w_far.at[far_rows((y + tall - k) % tall)], far_r.at[k])
            far_swap().start()

    @pl.when(sect == 0)
    def _():
        step_r(0, False)
        lax.fori_loop(0, batches, give_target, 0)
        for c in range(CHUNKS):
            step_f(0, c)
        step_r(1)

    @pl.when(upper)
    def _():
        for c in range(CHUNKS):
            step_f2(0, c)
        far_swap().wait_recv()

    def main(b, carry):
        more = b < batches - 1

        @pl.when(lower)
        def _():
            for c in range(CHUNKS):
                step_r2(b, c)

        @pl.when(more & (sect == 0) & (b > 0))
        def _():
            step_r(b + 1)

        def arrived(c):
            with jax.named_scope("c_wait"):
                @pl.when(sect == 0)
                def _():
                    gather_x(b, 0, c).wait_recv()
                    gather_x(b, 1, c).wait_recv()

                @pl.when(sect > 0)
                def _():
                    half_x(b, c).wait_recv()

        @pl.when(((sect == 0) | (lower & (sect == 2))) & (b > 0) & (core == 0))
        def _():
            pl.semaphore_signal(
                turn, inc=1, device_id={"segment": s, "dp": twin}, device_id_type=MESH
            )

        @pl.when(((sect == 0) | (lower & (sect == 2))) & (b > 0) & (core == 1))
        def _():
            pl.semaphore_wait(turn, 1)

        project(b, arrived)

        @pl.when((sect == 0) & (b == 0))
        def _():
            go_ahead()
        attend(b)

        @pl.when(lower)
        def _():
            mix_z(b, 1).start()

        @pl.when(sect == 0)
        def _():
            for w in range(WIDE):
                with jax.named_scope("out_dot"):
                    total = jnp.dot(mix[b], w_out[:, wide(w, WIDE)], preferred_element_type=F32)
                    pf[:, wide(w, WIDE)] = total
                    part[b, :, wide(w, WIDE)] = total.astype(BF16)
                for c in strips_of(w, WIDE):
                    sum_x(b, 0, c).start()
            for c in range(CHUNKS):
                sum_x(b, 1, c).start()


            @pl.when(more)
            def _():
                for c in range(CHUNKS):
                    step_f(b + 1, c)

            for c in range(CHUNKS):
                step_z(b, c)
            for c in range(CHUNKS):
                step_y(b, c)

        @pl.when(upper)
        def _():
            @pl.when(more)
            def _():
                for c in range(EARLY):
                    step_f2(b + 1, c)

            with jax.named_scope("mix_wait"):
                mix_z(b, 0).wait_recv()
                mix_z(b, 1).wait_recv()
            for w in range(WIDE):
                with jax.named_scope("out_dot2"):
                    total = jnp.dot(mix[b], w_out[:, wide(w, WIDE)], preferred_element_type=F32)
                    total = total + jnp.dot(mix_far[b], w_far[:, wide(w, WIDE)], preferred_element_type=F32)
                    pf[:, wide(w, WIDE)] = total
                    part[b, :, wide(w, WIDE)] = total.astype(BF16)
                for c in strips_of(w, WIDE):
                    sum_half(b, c).start()

            @pl.when(b == 0)
            def _():
                for c in range(CHUNKS):
                    step_y2(b, c)
                    if c > 0:
                        step_f2(b + 1, c - 1)
                step_f2(b + 1, CHUNKS - 1)

            @pl.when(b > 0)
            def _():
                for c in range(CHUNKS):
                    @pl.when(more)
                    def _():
                        step_f2(b + 1, c)

                    step_y2(b, c)
        return carry

    lax.fori_loop(0, batches, main, 0)

    def finish(b, carry):
        @pl.when((sect == 0) | ((sect == 1) & (b > 1)))
        def _():
            scattered(src, arr, src_s, src_r, 0, b)

        scattered(tgt, tg, tgt_s, tgt_r, 2 * GROUP, b)
        for c in range(CHUNKS):
            @pl.when(sect == 0)
            def _():
                sum_x(b, 0, c).wait_send()
                sum_x(b, 1, c).wait_send()
                sum_z(b, c).wait_send()
                gather_z(b, c).wait_send()
                gather_x(b, 0, c).wait_send()
                gather_x(b, 1, c).wait_send()
                relay_first(b, c).wait_send()

            @pl.when(lower)
            def _():
                lift_z(b, c).wait_send()
                half_x(b, c).wait_send()

            @pl.when(upper)
            def _():
                half_x(b, c).wait_send()
                sum_half(b, c).wait_send()

            @pl.when(upper & (sect < last))
            def _():
                relay(b, c).wait_send()

        @pl.when(lower)
        def _():
            mix_z(b, 0).wait_send()
            mix_z(b, 1).wait_send()

        @pl.when(sect == 2)
        def _():
            target_z(b).wait_send()
            target_x(b, 0).wait_send()
            target_x(b, 1).wait_send()

        @pl.when(upper & (sect == last))
        def _():
            def one(t, inner):
                @pl.when((t != s) | swap)
                def _():
                    out_copy(b, t).wait_send()
                return inner

            lax.fori_loop(0, n_seg, one, 0)

        with jax.named_scope("o_wait"):
            wait_for(out.at[b], out_r.at[b])
        return carry

    lax.fori_loop(0, batches, finish, 0)

    @pl.when(lower)
    def _():
        far_copy().wait_send()

    @pl.when(upper)
    def _():
        far_swap().wait_send()
        for k in range(1, tall):
            far_side(k).wait_send()


def on_device(n_seg, n_dp, src, tgt, slen, tlen, win, wout, gain, fgain):
    batches, seq, cols = src.shape
    width = cols * n_seg
    depth, fan = win.shape[1:]
    heads = wout.shape[1]
    rows = seq // GROUP
    any_space = pl.BlockSpec(memory_space=pl.ANY)
    vmem = pl.BlockSpec(memory_space=pltpu.VMEM)
    smem = pl.BlockSpec(memory_space=pltpu.SMEM)
    dma = pltpu.SemaphoreType.DMA
    return pl.pallas_call(
        functools.partial(kernel, n_seg, n_dp),
        out_shape=jax.ShapeDtypeStruct((batches, seq, cols), BF16),
        in_specs=[any_space, any_space, smem, smem, any_space, any_space, vmem, vmem],
        out_specs=any_space,
        scratch_shapes=[
            pltpu.VMEM((depth, fan), BF16),
            pltpu.VMEM((heads, width), BF16),
            pltpu.VMEM((heads, width), BF16),
            pltpu.VMEM((2 * batches, 128), F32),
            pltpu.VMEM((2 * batches, 128), F32),
            pltpu.VMEM((2 * batches, 128), F32),
            pltpu.VMEM((batches, seq, width), BF16),
            pltpu.VMEM((batches, seq, width), BF16),
            pltpu.VMEM((seq, width), BF16),
            pltpu.VMEM((batches, seq, heads), BF16),
            pltpu.VMEM((seq, fan), F32),
            pltpu.VMEM((seq, fan), BF16),
            pltpu.VMEM((batches, seq, heads), BF16),
            pltpu.VMEM((batches, seq, heads), BF16),
            pltpu.VMEM((seq, width), F32),
            pltpu.VMEM((batches, seq, width), BF16),
            pltpu.VMEM((batches, 2 * rows, width), BF16),
            pltpu.VMEM((batches, rows, width), BF16),
            pltpu.VMEM((batches, rows, width), BF16),
            pltpu.VMEM((batches, 2 * rows, width), BF16),
            pltpu.SemaphoreType.REGULAR, pltpu.SemaphoreType.REGULAR, dma((2,)), dma, dma, dma((n_dp // 4 + 1,)), dma((n_dp // 4 + 1,)), dma((batches, 2)), dma((batches, 2)),
            dma((batches, GROUP)), dma((batches, GROUP)), dma((batches,)), dma((batches,)),
            dma((batches,)), dma((batches,)), dma((batches, 2)), dma((batches, 2)),
            dma((batches, CHUNKS)), dma((batches, CHUNKS)),
            dma((batches, CHUNKS)), dma((batches, CHUNKS)),
            dma((batches, 2, CHUNKS)), dma((batches, 2, CHUNKS)),
            dma((batches, 2, CHUNKS)), dma((batches, 2, CHUNKS)),
            dma((batches, CHUNKS)), dma((batches, CHUNKS)),
            dma((batches, n_seg)), dma((batches,)),
        ],
        compiler_params=pltpu.CompilerParams(
            collective_id=0, has_side_effects=True, vmem_limit_bytes=56 * 1024 * 1024
        ),
    )(src, tgt, slen, tlen, win, wout, gain, fgain.reshape(1, -1))


def solution(mesh):
    spec = P("dp", None, "segment")
    return jax.shard_map(
        functools.partial(on_device, mesh.shape["segment"], mesh.shape["dp"]),
        mesh=mesh,
        in_specs=(spec, spec, P("dp"), P("dp"), P("segment", None, None), P("segment", None, None), P(), P()),
        out_specs=spec,
        check_vma=False,
    )
```
